8 devices in a mesh: dp: 1 (over z), tp: 2 (over y), cp: 4 (over x, core).
Axes of the slice: x: 2, y: 2, z: 1, core: 2. Of those that a mesh axis runs over, the one named last changes fastest.
Arguments:
- hidden: bfloat16 [1024, 4096], P(('dp', 'cp'))
- positions: int32 [1024], P(('dp', 'cp'))
- norm_gain: bfloat16 [4096], replicated
- w_query: bfloat16 [4096, 4096], P(None, 'tp')
- w_key: bfloat16 [4096, 1024], P(None, 'tp')
- w_value: bfloat16 [4096, 1024], P(None, 'tp')
- w_out: bfloat16 [4096, 4096], P('tp')
Outputs:
- output 1: bfloat16 [1024, 4096], P(('dp', 'cp'))
- output 2: bfloat16 [1024, 8, 128], P(('dp', 'cp'), 'tp')
- output 3: bfloat16 [1024, 8, 128], P(('dp', 'cp'), 'tp')
All inputs are finite; a program needn't handle non-finite values.
Results may differ from the reference program's by a relative error of at most 0.00808662.
Values are sent between devices in bfloat16 or wider.
A program may use at most 1 GiB of HBM per device.

```python
import math
import jax
import jax.numpy as jnp
from jax import lax

D = 4096
HEADS = 32
KV_HEADS = 8
HEAD = 128
SEQ = 1024
Q_ROWS = 128

EPS = 1e-5
LOG_THETA = math.log(1000000.0)


def setup_inputs(seed: int = 0, part: int = 0) -> dict:
    base_key = jax.random.key(seed)
    shared = jax.random.split(base_key, 5)
    part_keys = jax.random.split(jax.random.fold_in(base_key, part), 3)
    sharpness = math.sqrt(math.log(SEQ / 16.0))
    hidden = 0.5 * jax.random.normal(part_keys[0], (SEQ, D), jnp.float32)
    first_pos = jax.random.randint(part_keys[1], (), 0, SEQ, dtype=jnp.int32)
    pos_steps = jax.random.randint(part_keys[2], (SEQ,), 1, 3, dtype=jnp.int32)
    positions = (first_pos + jnp.cumsum(pos_steps) - 1).astype(jnp.int32)
    norm_gain = 1.0 + 0.3 * jax.random.normal(shared[0], (D,), jnp.float32)
    w_query = (sharpness / math.sqrt(D)) * jax.random.normal(shared[1], (D, HEADS * HEAD), jnp.float32)
    w_key = jax.random.normal(shared[2], (D, KV_HEADS * HEAD), jnp.float32) / math.sqrt(D)
    w_value = jax.random.normal(shared[3], (D, KV_HEADS * HEAD), jnp.float32) / math.sqrt(D)
    w_out = jax.random.normal(shared[4], (HEADS * HEAD, D), jnp.float32) / math.sqrt(HEADS * HEAD)
    return {
        'hidden': hidden.astype(jnp.bfloat16),
        'positions': positions,
        'norm_gain': norm_gain.astype(jnp.bfloat16),
        'w_query': w_query.astype(jnp.bfloat16),
        'w_key': w_key.astype(jnp.bfloat16),
        'w_value': w_value.astype(jnp.bfloat16),
        'w_out': w_out.astype(jnp.bfloat16),
    }


def rope_tables(positions):
    half_dim = HEAD // 2
    inv_freq = jnp.exp(jnp.arange(half_dim, dtype=jnp.float32) * (-2.0 * LOG_THETA / HEAD))
    angles = positions.astype(jnp.float32)[..., None] * inv_freq
    return jnp.cos(angles), jnp.sin(angles)


def apply_rope(head_vals, cos_t, sin_t):
    half_dim = HEAD // 2
    first_half = head_vals[..., :half_dim]
    second_half = head_vals[..., half_dim:]
    return jnp.concatenate([first_half * cos_t - second_half * sin_t, second_half * cos_t + first_half * sin_t], axis=-1)


def reference(hidden, positions, norm_gain, w_query, w_key, w_value, w_out):
    group_size = HEADS // KV_HEADS
    tile_count = SEQ // Q_ROWS
    hidden_f = hidden.astype(jnp.float32)
    inv_rms = lax.rsqrt(jnp.mean(hidden_f * hidden_f, axis=-1, keepdims=True) + EPS)
    normed = (hidden_f * inv_rms * norm_gain.astype(jnp.float32)).astype(jnp.bfloat16)
    cos_t, sin_t = rope_tables(positions)
    cos_b = cos_t[:, None, :]
    sin_b = sin_t[:, None, :]
    q_proj = jnp.dot(normed, w_query, preferred_element_type=jnp.float32).reshape(SEQ, HEADS, HEAD)
    k_proj = jnp.dot(normed, w_key, preferred_element_type=jnp.float32).reshape(SEQ, KV_HEADS, HEAD)
    queries = apply_rope(q_proj, cos_b, sin_b).astype(jnp.bfloat16)
    k_rope = apply_rope(k_proj, cos_b, sin_b).astype(jnp.bfloat16)
    values = jnp.dot(normed, w_value, preferred_element_type=jnp.float32).astype(jnp.bfloat16).reshape(SEQ, KV_HEADS, HEAD)
    q_tiles = queries.astype(jnp.float32).reshape(tile_count, Q_ROWS, KV_HEADS, group_size, HEAD)
    pos_tiles = positions.reshape(tile_count, Q_ROWS)
    k_full = k_rope.astype(jnp.float32)
    v_full = values.astype(jnp.float32)
    score_scale = 1.0 / math.sqrt(HEAD)

    def one_tile(tile_in):
        q_tile, q_pos = tile_in
        scores = jnp.einsum('qngd,knd->ngqk', q_tile, k_full) * score_scale
        visible = positions[None, :] <= q_pos[:, None]
        scores = jnp.where(visible, scores, -jnp.inf)
        weights = jax.nn.softmax(scores, axis=-1)
        return jnp.einsum('ngqk,knd->qngd', weights, v_full)

    attn_tiles = lax.map(one_tile, (q_tiles, pos_tiles))
    attn_o = attn_tiles.reshape(SEQ, HEADS * HEAD).astype(jnp.bfloat16)
    attn_sum = jnp.dot(attn_o, w_out, preferred_element_type=jnp.float32)
    hidden_out = (hidden_f + attn_sum).astype(jnp.bfloat16)
    return hidden_out, k_rope, values
```

```python
import functools
import math

import jax
import jax.numpy as jnp
from jax import lax
from jax.experimental import pallas as pl
from jax.experimental.pallas import tpu as pltpu
from jax.sharding import PartitionSpec as P

HEAD = 128
HALF = HEAD // 2
EPS = 1e-5
LOG_THETA = math.log(1000000.0)
SCORE_SCALE = 1.0 / math.sqrt(HEAD)
EXP2_SCALE = SCORE_SCALE / math.log(2.0)
MESH = pl.DeviceIdType.MESH
ROWS = 256
WIDTH = 4096
KV = 4
GROUP = 4
QCOLS = GROUP * HEAD
OCHUNK = 256
NOUT = WIDTH // OCHUNK
X_PARTS = 4
X_ROWS = ROWS // X_PARTS
NORM_ROWS = 16
F32 = jnp.float32
BF16 = jnp.bfloat16


def copies(refs):
    (x_hbm, pos_hbm, g_hbm, wq_hbm, wk_hbm, wv_hbm, wo_hbm, x_v, pos_v, g_v, wkv_v, wq_v, wo_v, x_sem, small_sem, wkv_sem, wq_sem, wo_sem) = refs

    def x_part(i):
        return pltpu.make_async_copy(x_hbm.at[pl.ds(i * X_ROWS, X_ROWS)], x_v.at[pl.ds(i * X_ROWS, X_ROWS)], x_sem.at[i])

    def wk_part(h):
        return pltpu.make_async_copy(wk_hbm.at[:, pl.ds(h * HEAD, HEAD)], wkv_v.at[h, :, pl.ds(0, HEAD)], wkv_sem.at[0, h])

    def wv_part(h):
        return pltpu.make_async_copy(wv_hbm.at[:, pl.ds(h * HEAD, HEAD)], wkv_v.at[h, :, pl.ds(HEAD, HEAD)], wkv_sem.at[1, h])

    def wq_part(j):
        return pltpu.make_async_copy(wq_hbm.at[:, pl.ds(j * QCOLS, QCOLS)], wq_v.at[j], wq_sem.at[j])

    def wo_part(n):
        cols = pl.ds(pl.multiple_of(n * OCHUNK, OCHUNK), OCHUNK)
        return pltpu.make_async_copy(wo_hbm.at[:, cols], wo_v.at[n], wo_sem.at[n])

    pos_copy = pltpu.make_async_copy(pos_hbm, pos_v, small_sem.at[0])
    g_copy = pltpu.make_async_copy(g_hbm, g_v, small_sem.at[1])
    return x_part, wk_part, wv_part, wq_part, wo_part, pos_copy, g_copy


def rope_tables(pos_v, cos_v, sin_v):
    lane = lax.broadcasted_iota(jnp.int32, (1, HEAD), 1)
    inv_freq = jnp.exp(lax.rem(lane, HALF).astype(F32) * (-2.0 * LOG_THETA / HEAD))
    low = lane < HALF
    top = jnp.broadcast_to(pos_v[pl.ds(0, HEAD)].reshape(1, HEAD).astype(F32), (HEAD, HEAD)).T
    bottom = jnp.broadcast_to(pos_v[pl.ds(HEAD, HEAD)].reshape(1, HEAD).astype(F32), (HEAD, HEAD)).T
    angles = jnp.where(low, top, bottom) * inv_freq
    cos_t, sin_t = jnp.cos(angles), jnp.sin(angles)
    cos_r, sin_r = pltpu.roll(cos_t, HALF, 1), pltpu.roll(sin_t, HALF, 1)
    cos_v[pl.ds(0, HEAD)] = jnp.where(low, cos_t, cos_r)
    cos_v[pl.ds(HEAD, HEAD)] = jnp.where(low, cos_r, cos_t)
    sin_v[pl.ds(0, HEAD)] = jnp.where(low, -sin_t, sin_r)
    sin_v[pl.ds(HEAD, HEAD)] = jnp.where(low, -sin_r, sin_t)


def rope(vals, cos_t, sin_t):
    return vals * cos_t + pltpu.roll(vals, HALF, 1) * sin_t


def attend(blocks, h, q_v, kv_v, o_v):
    row = lax.broadcasted_iota(jnp.int32, (ROWS, ROWS), 0)
    col = lax.broadcasted_iota(jnp.int32, (ROWS, ROWS), 1)
    for g in range(GROUP):
        q = q_v[h, pl.ds(g * ROWS, ROWS), :]
        scores = []
        for b in range(blocks):
            s = lax.dot_general(q, kv_v[b, h, :, pl.ds(0, HEAD)], (((1,), (1,)), ((), ())), preferred_element_type=F32)
            if b == blocks - 1:
                s = jnp.where(col <= row, s, -jnp.inf)
            scores.append(s)
        top = functools.reduce(jnp.maximum, [jnp.max(s, axis=-1, keepdims=True) for s in scores])
        base = top * EXP2_SCALE
        acc, total = None, None
        for b, s in enumerate(scores):
            p = jnp.exp2(s * EXP2_SCALE - base)
            part = jnp.sum(p, axis=-1, keepdims=True)
            pv = jnp.dot(p.astype(BF16), kv_v[b, h, :, pl.ds(HEAD, HEAD)], preferred_element_type=F32)
            total = part if total is None else total + part
            acc = pv if acc is None else acc + pv
        o_v[h, :, pl.ds(g * HEAD, HEAD)] = (acc / total).astype(BF16)


def kernel(x_hbm, pos_hbm, g_hbm, wq_hbm, wk_hbm, wv_hbm, wo_hbm,
           out_v, k_out, v_out,
           x_v, pos_v, g_v, wkv_v, wq_v, wo_v, h_v, cos_v, sin_v, kv_v, q_v, o_v, precv,
           x_sem, small_sem, wkv_sem, wq_sem, wo_sem, kv_send, kv_fwd, kv_recv, p_send, p_recv):
    tp, cp = lax.axis_index("tp"), lax.axis_index("cp")
    other = 1 - tp
    barrier = pltpu.get_barrier_semaphore()
    for t in range(2):
        for c in range(4):
            @pl.when((tp != t) | (cp != c))
            def _():
                pl.semaphore_signal(barrier, inc=1, device_id={"tp": t, "cp": c}, device_id_type=MESH)

    x_part, wk_part, wv_part, wq_part, wo_part, pos_copy, g_copy = copies(
        (x_hbm, pos_hbm, g_hbm, wq_hbm, wk_hbm, wv_hbm, wo_hbm, x_v, pos_v, g_v, wkv_v, wq_v, wo_v, x_sem, small_sem, wkv_sem, wq_sem, wo_sem))

    def start_wkv(h):
        wk_part(h).start()
        wv_part(h).start()

    pos_copy.start()
    g_copy.start()
    for i in range(X_PARTS):
        x_part(i).start()
    start_wkv(0)
    start_wkv(1)

    pos_copy.wait()
    rope_tables(pos_v, cos_v, sin_v)
    g_copy.wait()

    for i in range(X_PARTS):
        x_part(i).wait()

        def square(step, carry):
            rows = pl.ds(pl.multiple_of(i * X_ROWS + step * NORM_ROWS, NORM_ROWS), NORM_ROWS)
            xf = x_v[rows, :].astype(F32)
            mean = jnp.sum(xf * xf, axis=-1, keepdims=True) * (1.0 / WIDTH)
            inv = lax.rsqrt(mean + EPS)
            gain = g_v[...].reshape(1, WIDTH).astype(F32)
            h_v[rows, :] = (xf * inv * gain).astype(BF16)
            return carry

        lax.fori_loop(0, X_ROWS // NORM_ROWS, square, 0)
    start_wkv(2)
    start_wkv(3)

    pl.semaphore_wait(barrier, 7)

    def kv_copy(src_block, h, target, send):
        return pltpu.make_async_remote_copy(
            src_ref=kv_v.at[src_block, h], dst_ref=kv_v.at[src_block, h], send_sem=send.at[h],
            recv_sem=kv_recv.at[src_block, h], device_id={"cp": target}, device_id_type=MESH)

    def own_to(me, target, send, h):
        return kv_copy(me, h, target, send)

    cos_t, sin_t = cos_v[...], sin_v[...]
    hidden = h_v[...]
    for h in range(KV):
        wk_part(h).wait()
        wv_part(h).wait()
        wq_part(h).start()
        kv = jnp.dot(hidden, wkv_v[h], preferred_element_type=F32)
        k = rope(kv[:, :HEAD], cos_v[...], sin_v[...]).astype(BF16)
        v = kv[:, HEAD:].astype(BF16)
        kv_v[cp, h, :, pl.ds(0, HEAD)] = k
        kv_v[cp, h, :, pl.ds(HEAD, HEAD)] = v
        k_out[:, pl.ds(h * HEAD, HEAD)] = k
        v_out[:, pl.ds(h * HEAD, HEAD)] = v

        @pl.when(cp == 0)
        def _():
            own_to(0, 2, kv_send, h).start()
            own_to(0, 1, kv_fwd, h).start()

        @pl.when(cp == 1)
        def _():
            own_to(1, 3, kv_send, h).start()

        @pl.when(cp == 2)
        def _():
            own_to(2, 3, kv_send, h).start()

    def forward(h):
        @pl.when(cp == 2)
        def _():
            kv_copy(0, h, 2, kv_send).wait_recv()
            kv_copy(0, h, 3, kv_fwd).start()

        @pl.when(cp == 3)
        def _():
            kv_copy(1, h, 3, kv_send).wait_recv()
            kv_copy(1, h, 2, kv_fwd).start()

    for j in range(KV):
        wq_part(j).wait()
        for n in range(4):
            wo_part(j * 4 + n).start()
        qp = jnp.dot(hidden, wq_v[j], preferred_element_type=F32)
        for g in range(GROUP):
            q_v[j, pl.ds(g * ROWS, ROWS), :] = rope(qp[:, g * HEAD:(g + 1) * HEAD], cos_v[...], sin_v[...]).astype(BF16)
        if j >= 2:
            forward(j - 2)

    def arrive(src_block, h):
        kv_copy(src_block, h, 0, kv_send).wait_recv()

    @pl.when(cp == 0)
    def _():
        @pl.loop(0, KV)
        def _(h):
            attend(1, h, q_v, kv_v, o_v)

    @pl.when(cp == 1)
    def _():
        @pl.loop(0, KV)
        def _(h):
            arrive(0, h)
            attend(2, h, q_v, kv_v, o_v)

    @pl.when(cp == 2)
    def _():
        @pl.loop(0, KV)
        def _(h):
            arrive(1, h)
            attend(3, h, q_v, kv_v, o_v)

            @pl.when(h < 2)
            def _():
                kv_copy(0, h + 2, 2, kv_send).wait_recv()
                kv_copy(0, h + 2, 3, kv_fwd).start()

    @pl.when(cp == 3)
    def _():
        @pl.loop(0, KV)
        def _(h):
            arrive(0, h)
            arrive(2, h)
            attend(4, h, q_v, kv_v, o_v)

            @pl.when(h < 2)
            def _():
                kv_copy(1, h + 2, 3, kv_send).wait_recv()
                kv_copy(1, h + 2, 2, kv_fwd).start()

    def sent(n):
        return wkv_v.at[0, pl.ds(pl.multiple_of(n * ROWS, ROWS), ROWS), :]

    def p_copy(n):
        return pltpu.make_async_remote_copy(
            src_ref=sent(n), dst_ref=precv.at[n], send_sem=p_send.at[n], recv_sem=p_recv.at[n],
            device_id={"tp": other}, device_id_type=MESH)

    @pl.loop(0, NOUT)
    def _(n):
        wo_part(n).wait()
        part = None
        for h in range(KV):
            d = jnp.dot(o_v[h], wo_v[n, pl.ds(h * QCOLS, QCOLS), :], preferred_element_type=F32)
            part = d if part is None else part + d
        sent(n)[...] = part.astype(BF16)
        p_copy(n).start()

    @pl.loop(0, NOUT)
    def _(n):
        p_copy(n).wait_recv()
        cols = pl.ds(pl.multiple_of(n * OCHUNK, OCHUNK), OCHUNK)
        total = sent(n)[...].astype(F32) + precv[n].astype(F32)
        out_v[:, cols] = (x_v[:, cols].astype(F32) + total).astype(BF16)

    @pl.loop(0, NOUT)
    def _(n):
        p_copy(n).wait_send()

    @pl.loop(0, KV)
    def _(h):
        @pl.when(cp < 3)
        def _():
            kv_copy(0, h, 0, kv_send).wait_send()

        @pl.when((cp == 0) | (cp >= 2))
        def _():
            kv_copy(0, h, 0, kv_fwd).wait_send()


def solution(mesh):
    row_spec = P(('dp', 'cp'), None)
    cache_spec = P(('dp', 'cp'), 'tp', None)
    head_cols = P(None, 'tp')

    def local_block(hidden, positions, norm_gain, w_query, w_key, w_value, w_out):
        dma = pltpu.SemaphoreType.DMA
        out, k_rope, v_heads = pl.pallas_call(
            kernel,
            out_shape=[
                jax.ShapeDtypeStruct((ROWS, WIDTH), BF16),
                jax.ShapeDtypeStruct((ROWS, KV * HEAD), BF16),
                jax.ShapeDtypeStruct((ROWS, KV * HEAD), BF16),
            ],
            in_specs=[pl.BlockSpec(memory_space=pltpu.HBM)] * 7,
            out_specs=[pl.BlockSpec(memory_space=pltpu.VMEM)] * 3,
            scratch_shapes=[
                pltpu.VMEM((ROWS, WIDTH), BF16),
                pltpu.VMEM((ROWS,), jnp.int32),
                pltpu.VMEM((WIDTH,), BF16),
                pltpu.VMEM((KV, WIDTH, 2 * HEAD), BF16),
                pltpu.VMEM((KV, WIDTH, QCOLS), BF16),
                pltpu.VMEM((NOUT, KV * QCOLS, OCHUNK), BF16),
                pltpu.VMEM((ROWS, WIDTH), BF16),
                pltpu.VMEM((ROWS, HEAD), F32),
                pltpu.VMEM((ROWS, HEAD), F32),
                pltpu.VMEM((4, KV, ROWS, 2 * HEAD), BF16),
                pltpu.VMEM((KV, GROUP * ROWS, HEAD), BF16),
                pltpu.VMEM((KV, ROWS, QCOLS), BF16),
                pltpu.VMEM((NOUT, ROWS, OCHUNK), BF16),
                dma((X_PARTS,)), dma((2,)), dma((2, KV)), dma((KV,)), dma((NOUT,)),
                dma((KV,)), dma((KV,)), dma((4, KV)), dma((NOUT,)), dma((NOUT,)),
            ],
            compiler_params=pltpu.CompilerParams(collective_id=0, has_side_effects=True, vmem_limit_bytes=59 << 20),
        )(hidden, positions, norm_gain, w_query, w_key, w_value, w_out)
        return out, k_rope.reshape(ROWS, KV, HEAD), v_heads.reshape(ROWS, KV, HEAD)

    return jax.shard_map(local_block, mesh=mesh, in_specs=(row_spec, P(('dp', 'cp')), P(None), head_cols, head_cols, head_cols, P('tp', None)), out_specs=(row_spec, cache_spec, cache_spec), check_vma=False)
```

```python
import functools
import math

import jax
import jax.numpy as jnp
from jax import lax
from jax.experimental import pallas as pl
from jax.experimental.pallas import tpu as pltpu
from jax.sharding import PartitionSpec as P

HEAD = 128
HALF = HEAD // 2
EPS = 1e-5
LOG_THETA = math.log(1000000.0)
SCORE_SCALE = 1.0 / math.sqrt(HEAD)
EXP2_SCALE = SCORE_SCALE / math.log(2.0)
MESH = pl.DeviceIdType.MESH
ROWS = 256
WIDTH = 4096
KV = 4
GROUP = 4
QCOLS = GROUP * HEAD
OCHUNK = 256
NOUT = WIDTH // OCHUNK
X_PARTS = 4
X_ROWS = ROWS // X_PARTS
NORM_ROWS = 16
F32 = jnp.float32
BF16 = jnp.bfloat16


def wo_room(wq_v, n):
    deep = KV * QCOLS
    row = pl.multiple_of(lax.rem(n, 4) // 2 * deep, deep)
    col = pl.multiple_of(lax.rem(n, 2) * OCHUNK, OCHUNK)
    return wq_v.at[n // 4, pl.ds(row, deep), pl.ds(col, OCHUNK)]


def copies(refs):
    (x_hbm, pos_hbm, g_hbm, wq_hbm, wk_hbm, wv_hbm, wo_hbm, x_v, pos_v, g_v, wkv_v, wq_v, x_sem, small_sem, wkv_sem, wq_sem, wo_sem) = refs

    def x_part(i):
        return pltpu.make_async_copy(x_hbm.at[pl.ds(i * X_ROWS, X_ROWS)], x_v.at[pl.ds(i * X_ROWS, X_ROWS)], x_sem.at[i])

    def wk_part(h):
        return pltpu.make_async_copy(wk_hbm.at[:, pl.ds(h * HEAD, HEAD)], wkv_v.at[h, :, pl.ds(0, HEAD)], wkv_sem.at[0, h])

    def wv_part(h):
        return pltpu.make_async_copy(wv_hbm.at[:, pl.ds(h * HEAD, HEAD)], wkv_v.at[h, :, pl.ds(HEAD, HEAD)], wkv_sem.at[1, h])

    def wq_part(j):
        return pltpu.make_async_copy(wq_hbm.at[:, pl.ds(j * QCOLS, QCOLS)], wq_v.at[j], wq_sem.at[j])

    def wo_part(n):
        cols = pl.ds(pl.multiple_of(n * OCHUNK, OCHUNK), OCHUNK)
        return pltpu.make_async_copy(wo_hbm.at[:, cols], wo_room(wq_v, n), wo_sem.at[n])

    pos_copy = pltpu.make_async_copy(pos_hbm, pos_v, small_sem.at[0])
    g_copy = pltpu.make_async_copy(g_hbm, g_v, small_sem.at[1])
    return x_part, wk_part, wv_part, wq_part, wo_part, pos_copy, g_copy


def rope_tables(pos_v, cos_v, sin_v):
    lane = lax.broadcasted_iota(jnp.int32, (1, HEAD), 1)
    inv_freq = jnp.exp(lax.rem(lane, HALF).astype(F32) * (-2.0 * LOG_THETA / HEAD))
    low = lane < HALF
    top = jnp.broadcast_to(pos_v[pl.ds(0, HEAD)].reshape(1, HEAD).astype(F32), (HEAD, HEAD)).T
    bottom = jnp.broadcast_to(pos_v[pl.ds(HEAD, HEAD)].reshape(1, HEAD).astype(F32), (HEAD, HEAD)).T
    angles = jnp.where(low, top, bottom) * inv_freq
    cos_t, sin_t = jnp.cos(angles), jnp.sin(angles)
    cos_r, sin_r = pltpu.roll(cos_t, HALF, 1), pltpu.roll(sin_t, HALF, 1)
    cos_v[pl.ds(0, HEAD)] = jnp.where(low, cos_t, cos_r)
    cos_v[pl.ds(HEAD, HEAD)] = jnp.where(low, cos_r, cos_t)
    sin_v[pl.ds(0, HEAD)] = jnp.where(low, -sin_t, sin_r)
    sin_v[pl.ds(HEAD, HEAD)] = jnp.where(low, -sin_r, sin_t)


def rope(vals, cos_t, sin_t):
    return vals * cos_t + pltpu.roll(vals, HALF, 1) * sin_t


def attend(blocks, h, q_v, kv_v, o_v):
    row = lax.broadcasted_iota(jnp.int32, (ROWS, ROWS), 0)
    col = lax.broadcasted_iota(jnp.int32, (ROWS, ROWS), 1)
    for g in range(GROUP):
        q = q_v[h, pl.ds(g * ROWS, ROWS), :]
        scores = []
        for b in range(blocks):
            s = lax.dot_general(q, kv_v[b, h, :, pl.ds(0, HEAD)], (((1,), (1,)), ((), ())), preferred_element_type=F32)
            if b == blocks - 1:
                s = jnp.where(col <= row, s, -jnp.inf)
            scores.append(s)
        top = functools.reduce(jnp.maximum, [jnp.max(s, axis=-1, keepdims=True) for s in scores])
        base = top * EXP2_SCALE
        acc, total = None, None
        for b, s in enumerate(scores):
            p = jnp.exp2(s * EXP2_SCALE - base)
            part = jnp.sum(p, axis=-1, keepdims=True)
            pv = jnp.dot(p.astype(BF16), kv_v[b, h, :, pl.ds(HEAD, HEAD)], preferred_element_type=F32)
            total = part if total is None else total + part
            acc = pv if acc is None else acc + pv
        o_v[h, :, pl.ds(g * HEAD, HEAD)] = (acc / total).astype(BF16)


def kernel(x_hbm, pos_hbm, g_hbm, wq_hbm, wk_hbm, wv_hbm, wo_hbm,
           out_v, k_out, v_out,
           pos_v, g_v, wkv_v, wq_v, h_v, cos_v, sin_v, kv_v, q_v, o_v, precv, cache_v,
           x_sem, small_sem, wkv_sem, wq_sem, wo_sem, kv_send, kv_fwd, kv_recv, p_send, p_recv):
    tp, cp = lax.axis_index("tp"), lax.axis_index("cp")
    other = 1 - tp
    barrier = pltpu.get_barrier_semaphore()
    for t in range(2):
        for c in range(4):
            @pl.when((tp != t) | (cp != c))
            def _():
                pl.semaphore_signal(barrier, inc=1, device_id={"tp": t, "cp": c}, device_id_type=MESH)

    x_part, wk_part, wv_part, wq_part, wo_part, pos_copy, g_copy = copies(
        (x_hbm, pos_hbm, g_hbm, wq_hbm, wk_hbm, wv_hbm, wo_hbm, out_v, pos_v, g_v, wkv_v, wq_v, x_sem, small_sem, wkv_sem, wq_sem, wo_sem))

    def start_wkv(h):
        wk_part(h).start()
        wv_part(h).start()

    pos_copy.start()
    g_copy.start()
    for i in range(X_PARTS):
        x_part(i).start()
    start_wkv(0)
    start_wkv(1)

    pos_copy.wait()
    rope_tables(pos_v, cos_v, sin_v)
    g_copy.wait()

    for i in range(X_PARTS):
        x_part(i).wait()

        def square(step, carry):
            rows = pl.ds(pl.multiple_of(i * X_ROWS + step * NORM_ROWS, NORM_ROWS), NORM_ROWS)
            xf = out_v[rows, :].astype(F32)
            mean = jnp.sum(xf * xf, axis=-1, keepdims=True) * (1.0 / WIDTH)
            inv = lax.rsqrt(mean + EPS)
            gain = g_v[...].reshape(1, WIDTH).astype(F32)
            h_v[rows, :] = (xf * inv * gain).astype(BF16)
            return carry

        lax.fori_loop(0, X_ROWS // NORM_ROWS, square, 0)
    start_wkv(2)
    start_wkv(3)

    pl.semaphore_wait(barrier, 7)

    def kv_copy(src_block, h, target, send):
        return pltpu.make_async_remote_copy(
            src_ref=kv_v.at[src_block, h], dst_ref=kv_v.at[src_block, h], send_sem=send.at[h],
            recv_sem=kv_recv.at[src_block, h], device_id={"cp": target}, device_id_type=MESH)

    def own_to(me, target, send, h):
        return kv_copy(me, h, target, send)

    cos_t, sin_t = cos_v[...], sin_v[...]
    hidden = h_v[...]
    for h in range(KV):
        wk_part(h).wait()
        wv_part(h).wait()
        wq_part(h).start()
        kv = jnp.dot(hidden, wkv_v[h], preferred_element_type=F32)
        k = rope(kv[:, :HEAD], cos_v[...], sin_v[...]).astype(BF16)
        v = kv[:, HEAD:].astype(BF16)
        kv_v[cp, h, :, pl.ds(0, HEAD)] = k
        kv_v[cp, h, :, pl.ds(HEAD, HEAD)] = v

        @pl.when(cp == 0)
        def _():
            own_to(0, 2, kv_send, h).start()
            own_to(0, 1, kv_fwd, h).start()

        @pl.when(cp == 1)
        def _():
            own_to(1, 3, kv_send, h).start()

        @pl.when(cp == 2)
        def _():
            own_to(2, 3, kv_send, h).start()

    def forward(h):
        @pl.when(cp == 2)
        def _():
            kv_copy(0, h, 2, kv_send).wait_recv()
            kv_copy(0, h, 3, kv_fwd).start()

        @pl.when(cp == 3)
        def _():
            kv_copy(1, h, 3, kv_send).wait_recv()
            kv_copy(1, h, 2, kv_fwd).start()

    for j in range(KV):
        wq_part(j).wait()
        qp = jnp.dot(hidden, wq_v[j], preferred_element_type=F32)
        for g in range(GROUP):
            q_v[j, pl.ds(g * ROWS, ROWS), :] = rope(qp[:, g * HEAD:(g + 1) * HEAD], cos_v[...], sin_v[...]).astype(BF16)
        for n in range(4):
            wo_part(j * 4 + n).start()
        if j >= 2:
            forward(j - 2)

    def arrive(src_block, h):
        kv_copy(src_block, h, 0, kv_send).wait_recv()

    @pl.when(cp == 0)
    def _():
        @pl.loop(0, KV)
        def _(h):
            attend(1, h, q_v, kv_v, o_v)

    @pl.when(cp == 1)
    def _():
        @pl.loop(0, KV)
        def _(h):
            arrive(0, h)
            attend(2, h, q_v, kv_v, o_v)

    @pl.when(cp == 2)
    def _():
        @pl.loop(0, KV)
        def _(h):
            arrive(1, h)
            attend(3, h, q_v, kv_v, o_v)

            @pl.when(h < 2)
            def _():
                kv_copy(0, h + 2, 2, kv_send).wait_recv()
                kv_copy(0, h + 2, 3, kv_fwd).start()

    @pl.when(cp == 3)
    def _():
        @pl.loop(0, KV)
        def _(h):
            arrive(0, h)
            arrive(2, h)
            attend(4, h, q_v, kv_v, o_v)

            @pl.when(h < 2)
            def _():
                kv_copy(1, h + 2, 3, kv_send).wait_recv()
                kv_copy(1, h + 2, 2, kv_fwd).start()

    def sent(n):
        return wkv_v.at[0, pl.ds(pl.multiple_of(n * ROWS, ROWS), ROWS), :]

    def p_copy(n):
        return pltpu.make_async_remote_copy(
            src_ref=sent(n), dst_ref=precv.at[n], send_sem=p_send.at[n], recv_sem=p_recv.at[n],
            device_id={"tp": other}, device_id_type=MESH)

    @pl.loop(0, NOUT)
    def _(n):
        wo_part(n).wait()
        room = wo_room(wq_v, n)
        part = None
        for h in range(KV):
            d = jnp.dot(o_v[h], room[pl.ds(h * QCOLS, QCOLS), :], preferred_element_type=F32)
            part = d if part is None else part + d
        sent(n)[...] = part.astype(BF16)
        p_copy(n).start()

    for cache, lanes in ((k_out, pl.ds(0, HEAD)), (v_out, pl.ds(HEAD, HEAD))):
        for h in range(KV):
            cache_v[pl.ds(h, ROWS, stride=KV), :] = kv_v[cp, h, :, lanes].astype(F32)
        cache[...] = cache_v[...].astype(BF16)

    @pl.loop(0, NOUT)
    def _(n):
        p_copy(n).wait_recv()
        cols = pl.ds(pl.multiple_of(n * OCHUNK, OCHUNK), OCHUNK)
        total = sent(n)[...].astype(F32) + precv[n].astype(F32)
        out_v[:, cols] = (out_v[:, cols].astype(F32) + total).astype(BF16)

    @pl.loop(0, NOUT)
    def _(n):
        p_copy(n).wait_send()

    @pl.loop(0, KV)
    def _(h):
        @pl.when(cp < 3)
        def _():
            kv_copy(0, h, 0, kv_send).wait_send()

        @pl.when((cp == 0) | (cp >= 2))
        def _():
            kv_copy(0, h, 0, kv_fwd).wait_send()


def store_results(out_v, k_v, v_v, out_hbm, k_hbm, v_hbm, sem):
    stores = [pltpu.make_async_copy(src, dst, sem.at[i]) for i, (src, dst) in enumerate(((out_v, out_hbm), (k_v, k_hbm), (v_v, v_hbm)))]
    for store in stores:
        store.start()
    for store in stores:
        store.wait()


def solution(mesh):
    row_spec = P(('dp', 'cp'), None)
    cache_spec = P(('dp', 'cp'), 'tp', None)
    head_cols = P(None, 'tp')

    def local_block(hidden, positions, norm_gain, w_query, w_key, w_value, w_out):
        dma = pltpu.SemaphoreType.DMA
        out, k_rope, v_heads = pl.pallas_call(
            kernel,
            out_shape=[
                jax.ShapeDtypeStruct((ROWS, WIDTH), BF16),
                jax.ShapeDtypeStruct((ROWS * KV, HEAD), BF16),
                jax.ShapeDtypeStruct((ROWS * KV, HEAD), BF16),
            ],
            in_specs=[pl.BlockSpec(memory_space=pltpu.HBM)] * 7,
            out_specs=[pl.BlockSpec(memory_space=pltpu.VMEM)] * 3,
            scratch_shapes=[
                pltpu.VMEM((ROWS,), jnp.int32),
                pltpu.VMEM((WIDTH,), BF16),
                pltpu.VMEM((KV, WIDTH, 2 * HEAD), BF16),
                pltpu.VMEM((KV, WIDTH, QCOLS), BF16),
                pltpu.VMEM((ROWS, WIDTH), BF16),
                pltpu.VMEM((ROWS, HEAD), F32),
                pltpu.VMEM((ROWS, HEAD), F32),
                pltpu.VMEM((4, KV, ROWS, 2 * HEAD), BF16),
                pltpu.VMEM((KV, GROUP * ROWS, HEAD), BF16),
                pltpu.VMEM((KV, ROWS, QCOLS), BF16),
                pltpu.VMEM((NOUT, ROWS, OCHUNK), BF16),
                pltpu.VMEM((ROWS * KV, HEAD), F32),
                dma((X_PARTS,)), dma((2,)), dma((2, KV)), dma((KV,)), dma((NOUT,)),
                dma((KV,)), dma((KV,)), dma((4, KV)), dma((NOUT,)), dma((NOUT,)),
            ],
            compiler_params=pltpu.CompilerParams(collective_id=0, has_side_effects=True, vmem_limit_bytes=48 << 20),
        )(*(pltpu.with_memory_space_constraint(a, pltpu.HBM) for a in (hidden, positions, norm_gain, w_query, w_key, w_value, w_out)))
        out, k_rope, v_heads = pl.pallas_call(
            store_results,
            out_shape=[jax.ShapeDtypeStruct(a.shape, BF16) for a in (out, k_rope, v_heads)],
            in_specs=[pl.BlockSpec(memory_space=pltpu.VMEM)] * 3,
            out_specs=[pl.BlockSpec(memory_space=pl.ANY)] * 3,
            scratch_shapes=[dma((3,))],
            compiler_params=pltpu.CompilerParams(vmem_limit_bytes=4 << 20),
        )(out, k_rope, v_heads)
        return out, k_rope.reshape(ROWS, KV, HEAD), v_heads.reshape(ROWS, KV, HEAD)

    return jax.shard_map(local_block, mesh=mesh, in_specs=(row_spec, P(('dp', 'cp')), P(None), head_cols, head_cols, head_cols, P('tp', None)), out_specs=(row_spec, cache_spec, cache_spec), check_vma=False)
```

```python
import functools
import math

import jax
import jax.numpy as jnp
from jax import lax
from jax.experimental import pallas as pl
from jax.experimental.pallas import tpu as pltpu
from jax.sharding import PartitionSpec as P

HEAD = 128
HALF = HEAD // 2
EPS = 1e-5
LOG_THETA = math.log(1000000.0)
SCORE_SCALE = 1.0 / math.sqrt(HEAD)
EXP2_SCALE = SCORE_SCALE / math.log(2.0)
MESH = pl.DeviceIdType.MESH
ROWS = 256
WIDTH = 4096
KV = 4
GROUP = 4
QCOLS = GROUP * HEAD
PAIR = 2 * HEAD
OCHUNK = 256
NOUT = WIDTH // OCHUNK
X_PARTS = 4
X_ROWS = ROWS // X_PARTS
NORM_COLS = 1024
SLICES = WIDTH // NORM_COLS
RELAY_STEP = 6
LAG = 3
DETOURS = 2
F32 = jnp.float32
BF16 = jnp.bfloat16


def wo_room(wq_v, n):
    deep = KV * QCOLS
    row = pl.multiple_of(lax.rem(n, 4) // 2 * deep, deep)
    col = pl.multiple_of(lax.rem(n, 2) * OCHUNK, OCHUNK)
    return wq_v.at[n // 4, pl.ds(row, deep), pl.ds(col, OCHUNK)]


def copies(refs):
    (x_hbm, pos_hbm, g_hbm, wq_hbm, wk_hbm, wv_hbm, wo_hbm, x_v, pos_v, g_v, wkv_v, wq_v, x_sem, small_sem, first_sem, wkv_sem, wq_sem, wo_sem) = refs

    def x_part(i):
        return pltpu.make_async_copy(x_hbm.at[pl.ds(i * X_ROWS, X_ROWS)], x_v.at[pl.ds(i * X_ROWS, X_ROWS)], x_sem.at[i])

    def wkv_slice(t):
        rows = pl.ds(t * NORM_COLS, NORM_COLS)
        return [pltpu.make_async_copy(w.at[rows, pl.ds(0, PAIR)], wkv_v.at[0, rows, pl.ds(a * PAIR, PAIR)], first_sem.at[a, t]) for a, w in enumerate((wk_hbm, wv_hbm))]

    def wk_part(i):
        return pltpu.make_async_copy(wk_hbm.at[:, pl.ds(i * PAIR, PAIR)], wkv_v.at[i, :, pl.ds(0, PAIR)], wkv_sem.at[0, i])

    def wv_part(i):
        return pltpu.make_async_copy(wv_hbm.at[:, pl.ds(i * PAIR, PAIR)], wkv_v.at[i, :, pl.ds(PAIR, PAIR)], wkv_sem.at[1, i])

    def wq_part(j):
        return pltpu.make_async_copy(wq_hbm.at[:, pl.ds(j * QCOLS, QCOLS)], wq_v.at[j], wq_sem.at[j])

    def wo_part(n):
        cols = pl.ds(pl.multiple_of(n * OCHUNK, OCHUNK), OCHUNK)
        return pltpu.make_async_copy(wo_hbm.at[:, cols], wo_room(wq_v, n), wo_sem.at[n])

    pos_copy = pltpu.make_async_copy(pos_hbm, pos_v, small_sem.at[0])
    g_copy = pltpu.make_async_copy(g_hbm, g_v, small_sem.at[1])
    return x_part, wkv_slice, wk_part, wv_part, wq_part, wo_part, pos_copy, g_copy


def rope_tables(pos_v, cos_v, sin_v):
    lane = lax.broadcasted_iota(jnp.int32, (1, HEAD), 1)
    inv_freq = jnp.exp(lax.rem(lane, HALF).astype(F32) * (-2.0 * LOG_THETA / HEAD))
    low = lane < HALF
    top = jnp.broadcast_to(pos_v[pl.ds(0, HEAD)].reshape(1, HEAD).astype(F32), (HEAD, HEAD)).T
    bottom = jnp.broadcast_to(pos_v[pl.ds(HEAD, HEAD)].reshape(1, HEAD).astype(F32), (HEAD, HEAD)).T
    angles = jnp.where(low, top, bottom) * inv_freq
    cos_t, sin_t = jnp.cos(angles), jnp.sin(angles)
    cos_r, sin_r = pltpu.roll(cos_t, HALF, 1), pltpu.roll(sin_t, HALF, 1)
    cos_v[pl.ds(0, HEAD)] = jnp.where(low, cos_t, cos_r)
    cos_v[pl.ds(HEAD, HEAD)] = jnp.where(low, cos_r, cos_t)
    sin_v[pl.ds(0, HEAD)] = jnp.where(low, -sin_t, sin_r)
    sin_v[pl.ds(HEAD, HEAD)] = jnp.where(low, -sin_r, sin_t)


def rope(vals, cos_t, sin_t):
    return vals * cos_t + pltpu.roll(vals, HALF, 1) * sin_t


def block_scores(b, h, q_v, kv_v):
    return lax.dot_general(kv_v[b, h, :, pl.ds(0, HEAD)], q_v[h], (((1,), (1,)), ((), ())), preferred_element_type=F32) * EXP2_SCALE


def weighted(weights, b, h, kv_v):
    return lax.dot_general(kv_v[b, h, :, pl.ds(HEAD, HEAD)], weights.astype(BF16), (((0,), (0,)), ((), ())), preferred_element_type=F32)


def store_heads(acc, total, h, o_v):
    vals = (acc / total).astype(BF16)
    for g in range(GROUP):
        o_v[h, :, pl.ds(g * HEAD, HEAD)] = vals[:, g * ROWS:(g + 1) * ROWS].T


def attend_own(me, h, q_v, kv_v, o_v, max_v, sum_v, acc_v):
    key = lax.broadcasted_iota(jnp.int32, (ROWS, GROUP * ROWS), 0)
    query = lax.rem(lax.broadcasted_iota(jnp.int32, (ROWS, GROUP * ROWS), 1), ROWS)
    scores = jnp.where(key <= query, block_scores(me, h, q_v, kv_v), -jnp.inf)
    top = jnp.max(scores, axis=0, keepdims=True)
    weights = jnp.exp2(scores - top)
    total = jnp.sum(weights, axis=0, keepdims=True)
    acc = weighted(weights, me, h, kv_v)
    max_v[h], sum_v[h], acc_v[h] = top, total, acc
    store_heads(acc, total, h, o_v)


def attend_earlier(first, end, last, h, q_v, kv_v, o_v, max_v, sum_v, acc_v):
    scores = [block_scores(b, h, q_v, kv_v) for b in range(first, end)]
    top = functools.reduce(jnp.maximum, [jnp.max(s, axis=0, keepdims=True) for s in scores], max_v[h])
    scale = jnp.exp2(max_v[h] - top)
    total, acc = sum_v[h] * scale, acc_v[h] * scale
    for b, s in enumerate(scores):
        weights = jnp.exp2(s - top)
        total = total + jnp.sum(weights, axis=0, keepdims=True)
        acc = acc + weighted(weights, first + b, h, kv_v)
    if last:
        store_heads(acc, total, h, o_v)
    else:
        max_v[h], sum_v[h], acc_v[h] = top, total, acc


def kernel(x_hbm, pos_hbm, g_hbm, wq_hbm, wk_hbm, wv_hbm, wo_hbm,
           out_v, k_out, v_out,
           pos_v, g_v, wkv_v, wq_v, h_v, gain_v, inv_v, cos_v, sin_v, kv_v, q_v, o_v, max_v, sum_v, acc_v, precv, relay_v, cache_v,
           x_sem, small_sem, first_sem, wkv_sem, wq_sem, wo_sem, kv_send, kv_fwd, kv_recv, p_send, p_recv, relay_send, relay_recv):
    tp, cp = lax.axis_index("tp"), lax.axis_index("cp")
    other = 1 - tp
    x_part, wkv_slice, wk_part, wv_part, wq_part, wo_part, pos_copy, g_copy = copies(
        (x_hbm, pos_hbm, g_hbm, wq_hbm, wk_hbm, wv_hbm, wo_hbm, out_v, pos_v, g_v, wkv_v, wq_v, x_sem, small_sem, first_sem, wkv_sem, wq_sem, wo_sem))

    pos_copy.start()
    for i in range(X_PARTS):
        x_part(i).start()
    g_copy.start()
    for copy in wkv_slice(0):
        copy.start()
    barrier = pltpu.get_barrier_semaphore()
    for t in range(2):
        for c in range(4):
            @pl.when((tp != t) | (cp != c))
            def _():
                pl.semaphore_signal(barrier, inc=1, device_id={"tp": t, "cp": c}, device_id_type=MESH)

    pos_copy.wait()
    for t in range(1, SLICES):
        for copy in wkv_slice(t):
            copy.start()
    rope_tables(pos_v, cos_v, sin_v)
    for i in range(X_PARTS):
        x_part(i).wait()
        if i == 1:
            wk_part(1).start()
            wv_part(1).start()
        rows = pl.ds(i * X_ROWS, X_ROWS)
        squares = None
        for t in range(WIDTH // HEAD):
            xf = out_v[rows, pl.ds(t * HEAD, HEAD)].astype(F32)
            squares = xf * xf if squares is None else squares + xf * xf
        inv_v[rows, :] = squares
    mean = jnp.sum(inv_v[...], axis=-1, keepdims=True) * (1.0 / WIDTH)
    inv_v[...] = jnp.broadcast_to(lax.rsqrt(mean + EPS), (ROWS, HEAD))
    g_copy.wait()
    gain_v[...] = g_v[...].astype(F32)

    def kv_copy(src_block, h, target, send):
        return pltpu.make_async_remote_copy(
            src_ref=kv_v.at[src_block, h], dst_ref=kv_v.at[src_block, h], send_sem=send.at[h],
            recv_sem=kv_recv.at[src_block, h], device_id={"cp": target}, device_id_type=MESH)

    def own_to(me, target, send, h):
        return kv_copy(me, h, target, send)

    def heads_of(acc, pair):
        for a in range(2):
            h = 2 * pair + a
            k = rope(acc[:, a * HEAD:(a + 1) * HEAD], cos_v[...], sin_v[...]).astype(BF16)
            kv_v[cp, h, :, pl.ds(0, HEAD)] = k
            kv_v[cp, h, :, pl.ds(HEAD, HEAD)] = acc[:, PAIR + a * HEAD:PAIR + (a + 1) * HEAD].astype(BF16)

    def send_heads(pair):
        for h in (2 * pair, 2 * pair + 1):
            @pl.when(cp == 0)
            def _():
                own_to(0, 2, kv_send, h).start()
                own_to(0, 1, kv_fwd, h).start()

            @pl.when(cp == 1)
            def _():
                own_to(1, 3, kv_send, h).start()

            @pl.when(cp == 2)
            def _():
                own_to(2, 3, kv_send, h).start()

    def query_heads(acc, j):
        for g in range(GROUP):
            q_v[j, pl.ds(g * ROWS, ROWS), :] = rope(acc[:, g * HEAD:(g + 1) * HEAD], cos_v[...], sin_v[...]).astype(BF16)

    def normalise(t):
        for u in range(NORM_COLS // HEAD):
            lanes = pl.ds(t * NORM_COLS + u * HEAD, HEAD)
            gain = gain_v[pl.ds(t * (NORM_COLS // HEAD) + u, 1), :]
            h_v[:, lanes] = (out_v[:, lanes].astype(F32) * inv_v[...] * gain).astype(BF16)

    acc = None
    normalise(0)
    for t in range(SLICES):
        cols = pl.ds(t * NORM_COLS, NORM_COLS)
        for copy in wkv_slice(t):
            copy.wait()
        if t == 1:
            wq_part(0).start()
        if t + 1 < SLICES:
            normalise(t + 1)
        d = jnp.dot(h_v[:, cols], wkv_v[0, cols, :], preferred_element_type=F32)
        acc = d if acc is None else acc + d
    wq_part(1).start()
    heads_of(acc, 0)
    pl.semaphore_wait(barrier, 7)
    send_heads(0)

    wk_part(1).wait()
    wv_part(1).wait()
    wq_part(2).start()
    pending = jnp.dot(h_v[...], wkv_v[1], preferred_element_type=F32)

    def forward(h):
        @pl.when(cp == 2)
        def _():
            kv_copy(0, h, 2, kv_send).wait_recv()
            kv_copy(0, h, 3, kv_fwd).start()

        @pl.when(cp == 3)
        def _():
            kv_copy(1, h, 3, kv_send).wait_recv()
            kv_copy(1, h, 2, kv_fwd).start()

    stats = (q_v, kv_v, o_v, max_v, sum_v, acc_v)
    for j in range(KV):
        wq_part(j).wait()
        if j == 0:
            wq_part(3).start()
        acc = jnp.dot(h_v[...], wq_v[j], preferred_element_type=F32)
        if j == 0:
            heads_of(pending, 1)
            send_heads(1)
        else:
            query_heads(pending, j - 1)
            attend_own(cp, j - 1, *stats)
        pending = acc
        for n in range(4):
            wo_part(j * 4 + n).start()
        if j == KV - 1:
            forward(0)
    query_heads(pending, KV - 1)
    attend_own(cp, KV - 1, *stats)
    forward(1)
    forward(2)

    def arrive(src_block, h):
        kv_copy(src_block, h, 0, kv_send).wait_recv()

    @pl.when(cp == 1)
    def _():
        @pl.loop(0, KV)
        def _(h):
            arrive(0, h)
            attend_earlier(0, 1, True, h, *stats)

    @pl.when(cp == 2)
    def _():
        @pl.loop(0, KV)
        def _(h):
            arrive(1, h)
            attend_earlier(0, 2, True, h, *stats)

            @pl.when(h == 1)
            def _():
                kv_copy(0, 3, 2, kv_send).wait_recv()
                kv_copy(0, 3, 3, kv_fwd).start()

    @pl.when(cp == 3)
    def _():
        @pl.loop(0, KV)
        def _(h):
            arrive(2, h)
            attend_earlier(2, 3, False, h, *stats)

            @pl.when(h == 1)
            def _():
                kv_copy(1, 3, 3, kv_send).wait_recv()
                kv_copy(1, 3, 2, kv_fwd).start()

        @pl.loop(0, KV)
        def _(h):
            arrive(0, h)
            attend_earlier(0, 2, True, h, *stats)

    def sent(n):
        return wkv_v.at[0, pl.ds(pl.multiple_of(n * ROWS, ROWS), ROWS), pl.ds(0, OCHUNK)]

    def p_copy(n):
        return pltpu.make_async_remote_copy(
            src_ref=sent(n), dst_ref=precv.at[n], send_sem=p_send.at[n], recv_sem=p_recv.at[n],
            device_id={"tp": other}, device_id_type=MESH)

    def relay_in(n):
        return pltpu.make_async_remote_copy(
            src_ref=sent(n), dst_ref=relay_v.at[n], send_sem=p_send.at[n], recv_sem=relay_recv.at[n],
            device_id={"tp": other, "cp": 1}, device_id_type=MESH)

    def relay_out(n):
        return pltpu.make_async_remote_copy(
            src_ref=relay_v.at[n], dst_ref=precv.at[n], send_sem=relay_send.at[n], recv_sem=p_recv.at[n],
            device_id={"cp": 3}, device_id_type=MESH)

    @pl.loop(0, NOUT)
    def _(n):
        wo_part(n).wait()
        room = wo_room(wq_v, n)
        part = None
        for h in range(KV):
            d = jnp.dot(o_v[h], room[pl.ds(h * QCOLS, QCOLS), :], preferred_element_type=F32)
            part = d if part is None else part + d
        sent(n)[...] = part.astype(BF16)
        detour = (cp == 3) & (n < DETOURS)

        @pl.when(detour)
        def _():
            relay_in(n).start()

        @pl.when(jnp.logical_not(detour))
        def _():
            p_copy(n).start()

    for cache, lanes in ((k_out, pl.ds(0, HEAD)), (v_out, pl.ds(HEAD, HEAD))):
        for h in range(KV):
            cache_v[pl.ds(h, ROWS, stride=KV), :] = kv_v[cp, h, :, lanes].astype(F32)
        cache[...] = cache_v[...].astype(BF16)

    for h in range(KV):
        @pl.when(cp < 3)
        def _():
            kv_copy(0, h, 0, kv_send).wait_send()

        @pl.when((cp == 0) | (cp >= 2))
        def _():
            kv_copy(0, h, 0, kv_fwd).wait_send()

    def nth(step):
        return lax.rem(step + DETOURS, NOUT)

    @pl.loop(0, NOUT)
    def _(step):
        n = nth(step)

        @pl.when(step >= LAG)
        def _():
            p_copy(nth(step - LAG)).wait_send()

        @pl.when((cp == 1) & (step == RELAY_STEP))
        def _():
            for i in range(DETOURS):
                relay_in(i).wait_recv()
                relay_out(i).start()

        @pl.when((cp == 1) & (step == NOUT - LAG))
        def _():
            for i in range(DETOURS):
                relay_out(i).wait_send()

        p_copy(n).wait_recv()
        cols = pl.ds(pl.multiple_of(n * OCHUNK, OCHUNK), OCHUNK)
        total = sent(n)[...].astype(F32) + precv[n].astype(F32)
        out_v[:, cols] = (out_v[:, cols].astype(F32) + total).astype(BF16)

    for step in range(NOUT - LAG, NOUT):
        p_copy((step + DETOURS) % NOUT).wait_send()


def store_results(out_v, k_v, v_v, out_hbm, k_hbm, v_hbm, sem):
    stores = [pltpu.make_async_copy(src, dst, sem.at[i]) for i, (src, dst) in enumerate(((out_v, out_hbm), (k_v, k_hbm), (v_v, v_hbm)))]
    for store in stores:
        store.start()
    for store in stores:
        store.wait()


def solution(mesh):
    row_spec = P(('dp', 'cp'), None)
    cache_spec = P(('dp', 'cp'), 'tp', None)
    head_cols = P(None, 'tp')

    def local_block(hidden, positions, norm_gain, w_query, w_key, w_value, w_out):
        dma = pltpu.SemaphoreType.DMA
        out, k_rope, v_heads = pl.pallas_call(
            kernel,
            out_shape=[
                jax.ShapeDtypeStruct((ROWS, WIDTH), BF16),
                jax.ShapeDtypeStruct((ROWS * KV, HEAD), BF16),
                jax.ShapeDtypeStruct((ROWS * KV, HEAD), BF16),
            ],
            in_specs=[pl.BlockSpec(memory_space=pltpu.HBM)] * 7,
            out_specs=[pl.BlockSpec(memory_space=pltpu.VMEM)] * 3,
            scratch_shapes=[
                pltpu.VMEM((ROWS,), jnp.int32),
                pltpu.VMEM((WIDTH // HEAD, HEAD), BF16),
                pltpu.VMEM((2, WIDTH, 2 * PAIR), BF16),
                pltpu.VMEM((KV, WIDTH, QCOLS), BF16),
                pltpu.VMEM((ROWS, WIDTH), BF16),
                pltpu.VMEM((WIDTH // HEAD, HEAD), F32),
                pltpu.VMEM((ROWS, HEAD), F32),
                pltpu.VMEM((ROWS, HEAD), F32),
                pltpu.VMEM((ROWS, HEAD), F32),
                pltpu.VMEM((4, KV, ROWS, 2 * HEAD), BF16),
                pltpu.VMEM((KV, GROUP * ROWS, HEAD), BF16),
                pltpu.VMEM((KV, ROWS, QCOLS), BF16),
                pltpu.VMEM((KV, 1, GROUP * ROWS), F32),
                pltpu.VMEM((KV, 1, GROUP * ROWS), F32),
                pltpu.VMEM((KV, HEAD, GROUP * ROWS), F32),
                pltpu.VMEM((NOUT, ROWS, OCHUNK), BF16),
                pltpu.VMEM((DETOURS, ROWS, OCHUNK), BF16),
                pltpu.VMEM((ROWS * KV, HEAD), F32),
                dma((X_PARTS,)), dma((2,)), dma((2, WIDTH // NORM_COLS)), dma((2, 2)), dma((KV,)), dma((NOUT,)),
                dma((KV,)), dma((KV,)), dma((4, KV)), dma((NOUT,)), dma((NOUT,)), dma((DETOURS,)), dma((DETOURS,)),
            ],
            compiler_params=pltpu.CompilerParams(collective_id=0, has_side_effects=True, vmem_limit_bytes=48 << 20),
        )(*(pltpu.with_memory_space_constraint(a, pltpu.HBM) for a in (hidden, positions, norm_gain.reshape(WIDTH // HEAD, HEAD), w_query, w_key, w_value, w_out)))
        out, k_rope, v_heads = pl.pallas_call(
            store_results,
            out_shape=[jax.ShapeDtypeStruct(a.shape, BF16) for a in (out, k_rope, v_heads)],
            in_specs=[pl.BlockSpec(memory_space=pltpu.VMEM)] * 3,
            out_specs=[pl.BlockSpec(memory_space=pl.ANY)] * 3,
            scratch_shapes=[dma((3,))],
            compiler_params=pltpu.CompilerParams(vmem_limit_bytes=4 << 20),
        )(out, k_rope, v_heads)
        return out, k_rope.reshape(ROWS, KV, HEAD), v_heads.reshape(ROWS, KV, HEAD)

    return jax.shard_map(local_block, mesh=mesh, in_specs=(row_spec, P(('dp', 'cp')), P(None), head_cols, head_cols, head_cols, P('tp', None)), out_specs=(row_spec, cache_spec, cache_spec), check_vma=False)
```

```python
import functools
import math

import jax
import jax.numpy as jnp
from jax import lax
from jax.experimental import pallas as pl
from jax.experimental.pallas import tpu as pltpu
from jax.sharding import PartitionSpec as P

HEAD = 128
HALF = HEAD // 2
EPS = 1e-5
LOG_THETA = math.log(1000000.0)
SCORE_SCALE = 1.0 / math.sqrt(HEAD)
EXP2_SCALE = SCORE_SCALE / math.log(2.0)
MESH = pl.DeviceIdType.MESH
ROWS = 256
WIDTH = 4096
KV = 4
GROUP = 4
QCOLS = GROUP * HEAD
PAIR = 2 * HEAD
OCHUNK = 256
NOUT = WIDTH // OCHUNK
X_PARTS = 4
X_ROWS = ROWS // X_PARTS
SLICE_ROWS = 1024
SLICES = WIDTH // SLICE_ROWS
KEY_ROWS = 32
DETOUR_ROWS = (256, 128)
DETOURS = len(DETOUR_ROWS)
F32 = jnp.float32
BF16 = jnp.bfloat16


def wo_room(wq_v, n):
    deep = KV * QCOLS
    row = pl.multiple_of(lax.rem(n, 4) // 2 * deep, deep)
    col = pl.multiple_of(lax.rem(n, 2) * OCHUNK, OCHUNK)
    return wq_v.at[n // 4, pl.ds(row, deep), pl.ds(col, OCHUNK)]


def wait_bytes(room, sem):
    pltpu.make_async_copy(room, room, sem).wait()


def copies(refs):
    (x_hbm, pos_hbm, g_hbm, wq_hbm, wk_hbm, wv_hbm, wo_hbm, x_v, pos_v, g_v, wkv_v, wq_v, x_sem, small_sem, first_sem, wkv_sem, wq_sem) = refs

    def x_part(i):
        return pltpu.make_async_copy(x_hbm.at[pl.ds(i * X_ROWS, X_ROWS)], x_v.at[pl.ds(i * X_ROWS, X_ROWS)], x_sem.at[i])

    def wkv_slice(t):
        rows = pl.ds(t * SLICE_ROWS, SLICE_ROWS)
        return [pltpu.make_async_copy(w.at[rows, pl.ds(0, PAIR)], wkv_v.at[0, rows, pl.ds(a * PAIR, PAIR)], first_sem.at[t]) for a, w in enumerate((wk_hbm, wv_hbm))]

    wkv_rest = [pltpu.make_async_copy(w.at[:, pl.ds(PAIR, PAIR)], wkv_v.at[1, :, pl.ds(a * PAIR, PAIR)], wkv_sem) for a, w in enumerate((wk_hbm, wv_hbm))]

    def wq_part(j):
        return pltpu.make_async_copy(wq_hbm.at[:, pl.ds(j * QCOLS, QCOLS)], wq_v.at[j], wq_sem.at[j])

    def wo_part(j):
        deep = KV * QCOLS
        parts = []
        for a in range(2):
            cols = pl.ds(pl.multiple_of((2 * j + a) * QCOLS, QCOLS), QCOLS)
            parts.append(pltpu.make_async_copy(wo_hbm.at[:, cols], wq_v.at[j, pl.ds(a * deep, deep), :], wq_sem.at[j]))
        return parts

    pos_copy = pltpu.make_async_copy(pos_hbm, pos_v, small_sem.at[0])
    g_copy = pltpu.make_async_copy(g_hbm, g_v, small_sem.at[1])
    return x_part, wkv_slice, wkv_rest, wq_part, wo_part, pos_copy, g_copy


def rope_tables(pos_v, cos_v, sin_v):
    lane = lax.broadcasted_iota(jnp.int32, (1, HEAD), 1)
    inv_freq = jnp.exp(lax.rem(lane, HALF).astype(F32) * (-2.0 * LOG_THETA / HEAD))
    low = lane < HALF
    top = jnp.broadcast_to(pos_v[pl.ds(0, HEAD)].reshape(1, HEAD).astype(F32), (HEAD, HEAD)).T
    bottom = jnp.broadcast_to(pos_v[pl.ds(HEAD, HEAD)].reshape(1, HEAD).astype(F32), (HEAD, HEAD)).T
    angles = jnp.where(low, top, bottom) * inv_freq
    cos_t, sin_t = jnp.cos(angles), jnp.sin(angles)
    cos_r, sin_r = pltpu.roll(cos_t, HALF, 1), pltpu.roll(sin_t, HALF, 1)
    cos_v[pl.ds(0, HEAD)] = jnp.where(low, cos_t, cos_r)
    cos_v[pl.ds(HEAD, HEAD)] = jnp.where(low, cos_r, cos_t)
    sin_v[pl.ds(0, HEAD)] = jnp.where(low, -sin_t, sin_r)
    sin_v[pl.ds(HEAD, HEAD)] = jnp.where(low, -sin_r, sin_t)


def rope(vals, cos_t, sin_t):
    return vals * cos_t + pltpu.roll(vals, HALF, 1) * sin_t


def attend(units, merge, last, q_v, kv_v, o_v, max_v, sum_v, acc_v, score_v, weight_v):
    tops, sums = {}, {}

    def room(h, count):
        return h * ROWS if count <= ROWS else h % 2 * 2 * ROWS

    def score_phase(unit):
        h, start, count, first, width, causal = unit
        lanes = pl.ds(first, width)
        s = lax.dot_general(kv_v[h, pl.ds(start, count), pl.ds(0, HEAD)], q_v[h, lanes, :], (((1,), (1,)), ((), ())), preferred_element_type=F32)
        parts = [(0, s)]
        if causal:
            key = lax.broadcasted_iota(jnp.int32, (HEAD, width), 0)
            query = lax.rem(lax.broadcasted_iota(jnp.int32, (HEAD, width), 1), HEAD)
            free = count - HEAD
            parts = ([(0, s[:free])] if free else []) + [(free, jnp.where(key <= query, s[free:], -jnp.inf))]
        tall = []
        for row, part in parts:
            score_v[pl.ds(room(h, count) + row, part.shape[0]), lanes] = part
            tall.append(jnp.max(part.reshape(part.shape[0] // 8, 8, width), axis=0))
        top = jnp.max(functools.reduce(jnp.maximum, tall), axis=0, keepdims=True) * EXP2_SCALE
        tops[h, first] = jnp.maximum(top, max_v[h, :, lanes]) if merge else top

    def weight_phase(unit):
        h, start, count, first, width, causal = unit
        lanes = pl.ds(first, width)
        total = None
        for c in range(count // KEY_ROWS):
            rows = pl.ds(room(h, count) + c * KEY_ROWS, KEY_ROWS)
            w = jnp.exp2(score_v[rows, lanes] * EXP2_SCALE - tops[h, first])
            part = jnp.sum(w.reshape(KEY_ROWS // 8, 8, width), axis=0)
            total = part if total is None else total + part
            weight_v[rows, lanes] = w.astype(BF16)
        sums[h, first] = total

    def value_phase(unit):
        h, start, count, first, width, causal = unit
        lanes = pl.ds(first, width)
        acc = lax.dot_general(kv_v[h, pl.ds(start, count), pl.ds(HEAD, HEAD)], weight_v[pl.ds(room(h, count), count), lanes], (((0,), (0,)), ((), ())), preferred_element_type=F32)
        total = jnp.sum(sums[h, first], axis=0, keepdims=True)
        if merge:
            scale = jnp.exp2(max_v[h, :, lanes] - tops[h, first])
            total, acc = sum_v[h, :, lanes] * scale + total, acc_v[h, :, lanes] * scale + acc
        if not (merge and last):
            max_v[h, :, lanes], sum_v[h, :, lanes], acc_v[h, :, lanes] = tops[h, first], total, acc
        if last:
            vals = (acc / total).astype(BF16)
            for i in range(width // HEAD):
                half, g = divmod(first // HEAD + i, GROUP)
                o_v[h, pl.ds(half * HEAD, HEAD), pl.ds(g * HEAD, HEAD)] = vals[:, i * HEAD:(i + 1) * HEAD].T

    for i in range(len(units) + 2):
        if i < len(units):
            score_phase(units[i])
        if 0 <= i - 1 < len(units):
            weight_phase(units[i - 1])
        if 0 <= i - 2 < len(units):
            value_phase(units[i - 2])


def own_units(start):
    return [(h, start, (half + 1) * HEAD, half * QCOLS, QCOLS, True) for h in range(KV) for half in range(2)]


def block_units(heads, first, end):
    return [(h, first * ROWS, (end - first) * ROWS, 0, GROUP * ROWS, False) for h in heads]


def kernel(x_hbm, pos_hbm, g_hbm, wq_hbm, wk_hbm, wv_hbm, wo_hbm,
           out_v, k_out, v_out,
           pos_v, g_v, wkv_v, wq_v, h_v, gain_v, inv_v, cos_v, sin_v, kv_v, q_v, o_v, max_v, sum_v, acc_v, score_v, weight_v, precv, relay_v, cache_v,
           x_sem, small_sem, first_sem, wkv_sem, wq_sem, kv_send, kv_recv, p_send, p_recv, relay_send, relay_recv):
    tp, cp = lax.axis_index("tp"), lax.axis_index("cp")
    other = 1 - tp
    x_part, wkv_slice, wkv_rest, wq_part, wo_part, pos_copy, g_copy = copies(
        (x_hbm, pos_hbm, g_hbm, wq_hbm, wk_hbm, wv_hbm, wo_hbm, out_v, pos_v, g_v, wkv_v, wq_v, x_sem, small_sem, first_sem, wkv_sem, wq_sem))

    g_copy.start()
    for i in range(X_PARTS):
        x_part(i).start()
    pos_copy.start()
    for t in range(SLICES // 2):
        for copy in wkv_slice(t):
            copy.start()
    barrier = pltpu.get_barrier_semaphore()
    for t in range(2):
        for c in range(4):
            @pl.when((tp != t) | (cp != c))
            def _():
                pl.semaphore_signal(barrier, inc=1, device_id={"tp": t, "cp": c}, device_id_type=MESH)

    def normalise(i):
        rows = pl.ds(i * X_ROWS, X_ROWS)
        inv = inv_v[rows, :]
        for t in range(WIDTH // HEAD):
            lanes = pl.ds(t * HEAD, HEAD)
            h_v[rows, lanes] = (out_v[rows, lanes].astype(F32) * inv * gain_v[pl.ds(t, 1), :]).astype(BF16)

    g_copy.wait()
    gain_v[...] = g_v[...].astype(F32)
    for i in range(X_PARTS):
        x_part(i).wait()
        if i == 0:
            for t in range(SLICES // 2, SLICES):
                for copy in wkv_slice(t):
                    copy.start()
        if i == 3:
            for copy in wkv_rest:
                copy.start()
        rows = pl.ds(i * X_ROWS, X_ROWS)
        squares = None
        for t in range(WIDTH // HEAD):
            xf = out_v[rows, pl.ds(t * HEAD, HEAD)].astype(F32)
            squares = xf * xf if squares is None else squares + xf * xf
        mean = jnp.sum(squares, axis=-1, keepdims=True) * (1.0 / WIDTH)
        if i:
            normalise(i - 1)
        inv_v[rows, :] = jnp.broadcast_to(lax.rsqrt(mean + EPS), (X_ROWS, HEAD))
    normalise(X_PARTS - 1)

    def piece(block, h):
        return kv_v.at[h, pl.ds(pl.multiple_of(block * ROWS, ROWS), ROWS), :]

    def kv_copy(src_block, h, target):
        return pltpu.make_async_remote_copy(
            src_ref=piece(src_block, h), dst_ref=piece(src_block, h), send_sem=kv_send,
            recv_sem=kv_recv.at[src_block, h], device_id={"cp": target}, device_id_type=MESH)

    def heads_of(acc, pair):
        for a in range(2):
            h = 2 * pair + a
            k = rope(acc[:, a * HEAD:(a + 1) * HEAD], cos_v[...], sin_v[...]).astype(BF16)
            piece(cp, h)[:, pl.ds(0, HEAD)] = k
            piece(cp, h)[:, pl.ds(HEAD, HEAD)] = acc[:, PAIR + a * HEAD:PAIR + (a + 1) * HEAD].astype(BF16)

    def send_heads(pair):
        for h in (2 * pair, 2 * pair + 1):
            @pl.when(cp == 0)
            def _():
                kv_copy(0, h, 2).start()
                kv_copy(0, h, 1).start()

            @pl.when(cp == 1)
            def _():
                kv_copy(1, h, 3).start()

            @pl.when(cp == 2)
            def _():
                kv_copy(2, h, 3).start()

    def query_heads(acc, j):
        for g in range(GROUP):
            q = rope(acc[:, g * HEAD:(g + 1) * HEAD], cos_v[...], sin_v[...]).astype(BF16)
            for half in range(2):
                q_v[j, pl.ds(half * QCOLS + g * HEAD, HEAD), :] = q[half * HEAD:(half + 1) * HEAD]

    pos_copy.wait()
    acc = None
    for part in range(4):
        for t in range(part * SLICES // 4, (part + 1) * SLICES // 4):
            wait_bytes(wkv_v.at[0, pl.ds(t * SLICE_ROWS, SLICE_ROWS), :], first_sem.at[t])
        if part == 0:
            wq_part(0).start()
        deep = pl.ds(part * WIDTH // 4, WIDTH // 4)
        d = jnp.dot(h_v[:, deep], wkv_v[0, deep, :], preferred_element_type=F32)
        acc = d if acc is None else acc + d
        if part == 0:
            rope_tables(pos_v, cos_v, sin_v)
    wq_part(1).start()
    heads_of(acc, 0)
    pl.semaphore_wait(barrier, 7)
    send_heads(0)

    wait_bytes(wkv_v.at[1], wkv_sem)
    wq_part(2).start()
    pending = jnp.dot(h_v[...], wkv_v[1], preferred_element_type=F32)

    def forward_to(block, h, target):
        kv_copy(block, h, target).wait_recv()
        kv_copy(block, h, target).start()

    def forward(h):
        @pl.when(cp == 2)
        def _():
            forward_to(0, h, 3)

        @pl.when(cp == 3)
        def _():
            forward_to(1, h, 2)

    stats = (q_v, kv_v, o_v, max_v, sum_v, acc_v, score_v, weight_v)
    for j in range(KV):
        wq_part(j).wait()
        if j == 0:
            wq_part(3).start()
        acc = jnp.dot(h_v[...], wq_v[j], preferred_element_type=F32)
        if j == 0:
            heads_of(pending, 1)
            send_heads(1)
        else:
            query_heads(pending, j - 1)
        pending = acc
        for copy in wo_part(j):
            copy.start()
        if j == KV - 1:
            forward(0)
    query_heads(pending, KV - 1)
    attend(own_units(pl.multiple_of(cp * ROWS, ROWS)), False, True, *stats)
    forward(1)

    def arrive(src_block, h):
        kv_copy(src_block, h, 0).wait_recv()

    @pl.when(cp == 1)
    def _():
        for h in range(KV):
            arrive(0, h)
        attend(block_units(range(KV), 0, 1), True, True, *stats)

    @pl.when(cp == 2)
    def _():
        arrive(1, 0)
        arrive(1, 1)
        attend(block_units((0, 1), 0, 2), True, True, *stats)
        forward_to(0, 2, 3)
        arrive(1, 2)
        attend(block_units((2,), 0, 2), True, True, *stats)
        forward_to(0, 3, 3)
        arrive(1, 3)
        attend(block_units((3,), 0, 2), True, True, *stats)

    @pl.when(cp == 3)
    def _():
        for h in range(KV):
            arrive(2, h)
        attend(block_units((0, 1), 2, 3), True, False, *stats)
        forward_to(1, 2, 2)
        attend(block_units((2, 3), 2, 3), True, False, *stats)
        arrive(0, 0)
        attend(block_units((0,), 0, 2), True, True, *stats)
        forward_to(1, 3, 2)
        arrive(0, 1)
        arrive(0, 2)
        attend(block_units((1, 2), 0, 2), True, True, *stats)
        arrive(0, 3)
        attend(block_units((3,), 0, 2), True, True, *stats)

    def sent(n):
        return wkv_v.at[0, pl.ds(pl.multiple_of(n * ROWS, ROWS), ROWS), pl.ds(0, OCHUNK)]

    def group(n):
        early = (n + 2) // 4
        return jnp.where(n < 14, early, n - 10) if not isinstance(n, int) else (early if n < 14 else n - 10)

    def p_copy(n):
        return pltpu.make_async_remote_copy(
            src_ref=sent(n), dst_ref=precv.at[n], send_sem=p_send, recv_sem=p_recv.at[group(n)],
            device_id={"tp": other}, device_id_type=MESH)

    def detour(i):
        return pl.ds(0, DETOUR_ROWS[i])

    def relay_in(i):
        return pltpu.make_async_remote_copy(
            src_ref=sent(i).at[detour(i)], dst_ref=relay_v.at[pl.ds(i * ROWS, DETOUR_ROWS[i])], send_sem=p_send, recv_sem=relay_recv,
            device_id={"tp": other, "cp": 1}, device_id_type=MESH)

    def relay_out(i):
        return pltpu.make_async_remote_copy(
            src_ref=relay_v.at[pl.ds(i * ROWS, DETOUR_ROWS[i])], dst_ref=precv.at[i, detour(i)], send_sem=relay_send, recv_sem=p_recv.at[group(i)],
            device_id={"cp": 3}, device_id_type=MESH)

    def rest(i):
        rows = pl.ds(DETOUR_ROWS[i], ROWS - DETOUR_ROWS[i])
        return pltpu.make_async_remote_copy(
            src_ref=sent(i).at[rows], dst_ref=precv.at[i, rows], send_sem=p_send, recv_sem=p_recv.at[group(i)],
            device_id={"tp": other}, device_id_type=MESH)

    @pl.loop(0, NOUT)
    def _(n):
        @pl.when(lax.rem(n, 4) == 0)
        def _():
            wait_bytes(wq_v.at[n // 4], wq_sem.at[n // 4])

        room = wo_room(wq_v, n)
        part = None
        for h in range(KV):
            d = jnp.dot(o_v[h], room[pl.ds(h * QCOLS, QCOLS), :], preferred_element_type=F32)
            part = d if part is None else part + d
        sent(n)[...] = part.astype(BF16)
        for i in range(DETOURS):
            @pl.when((cp == 3) & (n == i))
            def _():
                relay_in(i).start()
                if DETOUR_ROWS[i] < ROWS:
                    rest(i).start()

        @pl.when((cp < 3) | (n >= DETOURS))
        def _():
            p_copy(n).start()

    for cache, lanes in ((k_out, pl.ds(0, HEAD)), (v_out, pl.ds(HEAD, HEAD))):
        for h in range(KV):
            cache_v[pl.ds(h, ROWS, stride=KV), :] = piece(cp, h)[:, lanes].astype(F32)
        cache[...] = cache_v[...].astype(BF16)

    @pl.when(lax.rem(cp, 2) == 0)
    def _():
        wait_bytes(kv_v.at[:, pl.ds(0, 2 * ROWS), :], kv_send)

    @pl.when(lax.rem(cp, 2) == 1)
    def _():
        wait_bytes(kv_v.at[:, pl.ds(0, ROWS), :], kv_send)

    def add_chunks(first, count):
        wait_bytes(precv.at[pl.ds(first, count)], p_recv.at[group(first)])
        for n in range(first, first + count):
            cols = pl.ds(n * OCHUNK, OCHUNK)
            total = sent(n)[...].astype(F32) + precv[n].astype(F32)
            out_v[:, cols] = (out_v[:, cols].astype(F32) + total).astype(BF16)

    add_chunks(2, 4)
    add_chunks(6, 4)

    @pl.when(cp == 1)
    def _():
        wait_bytes(relay_v, relay_recv)
        for i in range(DETOURS):
            relay_out(i).start()

    add_chunks(10, 4)

    @pl.when(cp == 1)
    def _():
        wait_bytes(relay_v, relay_send)

    add_chunks(0, 2)
    add_chunks(14, 1)
    add_chunks(15, 1)
    wait_bytes(precv, p_send)


def store_results(out_v, k_v, v_v, out_hbm, k_hbm, v_hbm, sem):
    stores = [pltpu.make_async_copy(src, dst, sem.at[i]) for i, (src, dst) in enumerate(((out_v, out_hbm), (k_v, k_hbm), (v_v, v_hbm)))]
    for store in stores:
        store.start()
    for store in stores:
        store.wait()


def solution(mesh):
    row_spec = P(('dp', 'cp'), None)
    cache_spec = P(('dp', 'cp'), 'tp', None)
    head_cols = P(None, 'tp')

    def local_block(hidden, positions, norm_gain, w_query, w_key, w_value, w_out):
        dma = pltpu.SemaphoreType.DMA
        out, k_rope, v_heads = pl.pallas_call(
            kernel,
            out_shape=[
                jax.ShapeDtypeStruct((ROWS, WIDTH), BF16),
                jax.ShapeDtypeStruct((ROWS * KV, HEAD), BF16),
                jax.ShapeDtypeStruct((ROWS * KV, HEAD), BF16),
            ],
            in_specs=[pl.BlockSpec(memory_space=pltpu.HBM)] * 7,
            out_specs=[pl.BlockSpec(memory_space=pltpu.VMEM)] * 3,
            scratch_shapes=[
                pltpu.VMEM((ROWS,), jnp.int32),
                pltpu.VMEM((WIDTH // HEAD, HEAD), BF16),
                pltpu.VMEM((2, WIDTH, 2 * PAIR), BF16),
                pltpu.VMEM((KV, WIDTH, QCOLS), BF16),
                pltpu.VMEM((ROWS, WIDTH), BF16),
                pltpu.VMEM((WIDTH // HEAD, HEAD), F32),
                pltpu.VMEM((ROWS, HEAD), F32),
                pltpu.VMEM((ROWS, HEAD), F32),
                pltpu.VMEM((ROWS, HEAD), F32),
                pltpu.VMEM((KV, 4 * ROWS, 2 * HEAD), BF16),
                pltpu.VMEM((KV, GROUP * ROWS, HEAD), BF16),
                pltpu.VMEM((KV, ROWS, QCOLS), BF16),
                pltpu.VMEM((KV, 1, GROUP * ROWS), F32),
                pltpu.VMEM((KV, 1, GROUP * ROWS), F32),
                pltpu.VMEM((KV, HEAD, GROUP * ROWS), F32),
                pltpu.VMEM((KV * ROWS, GROUP * ROWS), F32),
                pltpu.VMEM((KV * ROWS, GROUP * ROWS), BF16),
                pltpu.VMEM((NOUT, ROWS, OCHUNK), BF16),
                pltpu.VMEM((sum(DETOUR_ROWS), OCHUNK), BF16),
                pltpu.VMEM((ROWS * KV, HEAD), F32),
                dma((X_PARTS,)), dma((2,)), dma((SLICES,)), dma, dma((KV,)),
                dma, dma((3, KV)), dma, dma((6,)), dma, dma,
            ],
            compiler_params=pltpu.CompilerParams(collective_id=0, has_side_effects=True, vmem_limit_bytes=49 << 20),
        )(*(pltpu.with_memory_space_constraint(a, pltpu.HBM) for a in (hidden, positions, norm_gain.reshape(WIDTH // HEAD, HEAD), w_query, w_key, w_value, w_out)))
        out, k_rope, v_heads = pl.pallas_call(
            store_results,
            out_shape=[jax.ShapeDtypeStruct(a.shape, BF16) for a in (out, k_rope, v_heads)],
            in_specs=[pl.BlockSpec(memory_space=pltpu.VMEM)] * 3,
            out_specs=[pl.BlockSpec(memory_space=pl.ANY)] * 3,
            scratch_shapes=[dma((3,))],
            compiler_params=pltpu.CompilerParams(vmem_limit_bytes=4 << 20),
        )(out, k_rope, v_heads)
        return out, k_rope.reshape(ROWS, KV, HEAD), v_heads.reshape(ROWS, KV, HEAD)

    return jax.shard_map(local_block, mesh=mesh, in_specs=(row_spec, P(('dp', 'cp')), P(None), head_cols, head_cols, head_cols, P('tp', None)), out_specs=(row_spec, cache_spec, cache_spec), check_vma=False)
```

```python
import functools
import math

import jax
import jax.numpy as jnp
from jax import lax
from jax.experimental import pallas as pl
from jax.experimental.pallas import tpu as pltpu
from jax.sharding import PartitionSpec as P

HEAD = 128
HALF = HEAD // 2
EPS = 1e-5
LOG_THETA = math.log(1000000.0)
SCORE_SCALE = 1.0 / math.sqrt(HEAD)
EXP2_SCALE = SCORE_SCALE / math.log(2.0)
MESH = pl.DeviceIdType.MESH
ROWS = 256
WIDTH = 4096
KV = 4
GROUP = 4
QCOLS = GROUP * HEAD
PAIR = 2 * HEAD
OCHUNK = 256
NOUT = WIDTH // OCHUNK
X_PARTS = 4
X_ROWS = ROWS // X_PARTS
SLICE_ROWS = 1024
SLICES = WIDTH // SLICE_ROWS
KEY_ROWS = 32
DETOUR_ROWS = {1: (256, 256, 256), 3: (256, 256, 256)}
F32 = jnp.float32
BF16 = jnp.bfloat16


def wo_room(wq_v, n):
    deep = KV * QCOLS
    row = pl.multiple_of(lax.rem(n, 4) // 2 * deep, deep)
    col = pl.multiple_of(lax.rem(n, 2) * OCHUNK, OCHUNK)
    return wq_v.at[n // 4, pl.ds(row, deep), pl.ds(col, OCHUNK)]


def wait_bytes(room, sem):
    pltpu.make_async_copy(room, room, sem).wait()


def copies(refs):
    (x_hbm, pos_hbm, g_hbm, wq_hbm, wk_hbm, wv_hbm, wo_hbm, x_v, pos_v, g_v, wkv_v, wq_v, x_sem, small_sem, first_sem, wkv_sem, wq_sem) = refs

    def x_part(i):
        return pltpu.make_async_copy(x_hbm.at[pl.ds(i * X_ROWS, X_ROWS)], x_v.at[pl.ds(i * X_ROWS, X_ROWS)], x_sem.at[i])

    def wkv_slice(t):
        rows = pl.ds(t * SLICE_ROWS, SLICE_ROWS)
        return [pltpu.make_async_copy(w.at[rows, pl.ds(0, PAIR)], wkv_v.at[0, rows, pl.ds(a * PAIR, PAIR)], first_sem.at[t]) for a, w in enumerate((wk_hbm, wv_hbm))]

    wkv_rest = [pltpu.make_async_copy(w.at[:, pl.ds(PAIR, PAIR)], wkv_v.at[1, :, pl.ds(a * PAIR, PAIR)], wkv_sem) for a, w in enumerate((wk_hbm, wv_hbm))]

    def wq_part(j):
        return pltpu.make_async_copy(wq_hbm.at[:, pl.ds(j * QCOLS, QCOLS)], wq_v.at[j], wq_sem.at[j])

    def wo_part(j):
        deep = KV * QCOLS
        parts = []
        for a in range(2):
            cols = pl.ds(pl.multiple_of((2 * j + a) * QCOLS, QCOLS), QCOLS)
            parts.append(pltpu.make_async_copy(wo_hbm.at[:, cols], wq_v.at[j, pl.ds(a * deep, deep), :], wq_sem.at[j]))
        return parts

    pos_copy = pltpu.make_async_copy(pos_hbm, pos_v, small_sem.at[0])
    g_copy = pltpu.make_async_copy(g_hbm, g_v, small_sem.at[1])
    return x_part, wkv_slice, wkv_rest, wq_part, wo_part, pos_copy, g_copy


def rope_tables(pos_v, cos_v, sin_v):
    lane = lax.broadcasted_iota(jnp.int32, (1, HEAD), 1)
    inv_freq = jnp.exp(lax.rem(lane, HALF).astype(F32) * (-2.0 * LOG_THETA / HEAD))
    low = lane < HALF
    top = jnp.broadcast_to(pos_v[pl.ds(0, HEAD)].reshape(1, HEAD).astype(F32), (HEAD, HEAD)).T
    bottom = jnp.broadcast_to(pos_v[pl.ds(HEAD, HEAD)].reshape(1, HEAD).astype(F32), (HEAD, HEAD)).T
    angles = jnp.where(low, top, bottom) * inv_freq
    cos_t, sin_t = jnp.cos(angles), jnp.sin(angles)
    cos_r, sin_r = pltpu.roll(cos_t, HALF, 1), pltpu.roll(sin_t, HALF, 1)
    cos_v[pl.ds(0, HEAD)] = jnp.where(low, cos_t, cos_r)
    cos_v[pl.ds(HEAD, HEAD)] = jnp.where(low, cos_r, cos_t)
    sin_v[pl.ds(0, HEAD)] = jnp.where(low, -sin_t, sin_r)
    sin_v[pl.ds(HEAD, HEAD)] = jnp.where(low, -sin_r, sin_t)


def rope(vals, cos_t, sin_t):
    return vals * cos_t + pltpu.roll(vals, HALF, 1) * sin_t


def attend(units, merge, last, q_v, kv_v, o_v, max_v, sum_v, acc_v, score_v, weight_v):
    tops, sums = {}, {}

    def room(h, count):
        return h * ROWS if count <= ROWS else h % 2 * 2 * ROWS

    def score_phase(unit):
        h, start, count, first, width, causal = unit
        lanes = pl.ds(first, width)
        s = lax.dot_general(kv_v[h, pl.ds(start, count), pl.ds(0, HEAD)], q_v[h, lanes, :], (((1,), (1,)), ((), ())), preferred_element_type=F32)
        parts = [(0, s)]
        if causal:
            key = lax.broadcasted_iota(jnp.int32, (HEAD, width), 0)
            query = lax.rem(lax.broadcasted_iota(jnp.int32, (HEAD, width), 1), HEAD)
            free = count - HEAD
            parts = ([(0, s[:free])] if free else []) + [(free, jnp.where(key <= query, s[free:], -jnp.inf))]
        tall = []
        for row, part in parts:
            score_v[pl.ds(room(h, count) + row, part.shape[0]), lanes] = part
            tall.append(jnp.max(part.reshape(part.shape[0] // 8, 8, width), axis=0))
        top = jnp.max(functools.reduce(jnp.maximum, tall), axis=0, keepdims=True) * EXP2_SCALE
        tops[h, first] = jnp.maximum(top, max_v[h, :, lanes]) if merge else top

    def weight_phase(unit):
        h, start, count, first, width, causal = unit
        lanes = pl.ds(first, width)
        total = None
        for c in range(count // KEY_ROWS):
            rows = pl.ds(room(h, count) + c * KEY_ROWS, KEY_ROWS)
            w = jnp.exp2(score_v[rows, lanes] * EXP2_SCALE - tops[h, first])
            part = jnp.sum(w.reshape(KEY_ROWS // 8, 8, width), axis=0)
            total = part if total is None else total + part
            weight_v[rows, lanes] = w.astype(BF16)
        sums[h, first] = total

    def value_phase(unit):
        h, start, count, first, width, causal = unit
        lanes = pl.ds(first, width)
        acc = lax.dot_general(kv_v[h, pl.ds(start, count), pl.ds(HEAD, HEAD)], weight_v[pl.ds(room(h, count), count), lanes], (((0,), (0,)), ((), ())), preferred_element_type=F32)
        total = jnp.sum(sums[h, first], axis=0, keepdims=True)
        if merge:
            scale = jnp.exp2(max_v[h, :, lanes] - tops[h, first])
            total, acc = sum_v[h, :, lanes] * scale + total, acc_v[h, :, lanes] * scale + acc
        if not (merge and last):
            max_v[h, :, lanes], sum_v[h, :, lanes], acc_v[h, :, lanes] = tops[h, first], total, acc
        if last:
            vals = (acc / total).astype(BF16)
            for i in range(width // HEAD):
                half, g = divmod(first // HEAD + i, GROUP)
                o_v[h, pl.ds(half * HEAD, HEAD), pl.ds(g * HEAD, HEAD)] = vals[:, i * HEAD:(i + 1) * HEAD].T

    for i in range(len(units) + 2):
        if i < len(units):
            score_phase(units[i])
        if 0 <= i - 1 < len(units):
            weight_phase(units[i - 1])
        if 0 <= i - 2 < len(units):
            value_phase(units[i - 2])


def own_units(start):
    return [(h, start, (half + 1) * HEAD, half * QCOLS, QCOLS, True) for h in range(KV) for half in range(2)]


def block_units(heads, first, end):
    return [(h, first * ROWS, (end - first) * ROWS, 0, GROUP * ROWS, False) for h in heads]


def kernel(x_hbm, pos_hbm, g_hbm, wq_hbm, wk_hbm, wv_hbm, wo_hbm,
           out_v, k_out, v_out,
           pos_v, g_v, wkv_v, wq_v, h_v, gain_v, inv_v, cos_v, sin_v, kv_v, q_v, o_v, max_v, sum_v, acc_v, score_v, weight_v, precv, relay_v, cache_v,
           x_sem, small_sem, first_sem, wkv_sem, wq_sem, kv_send, kv_recv, p_send, p_recv, relay_send, relay_recv):
    tp, cp = lax.axis_index("tp"), lax.axis_index("cp")
    other = 1 - tp
    x_part, wkv_slice, wkv_rest, wq_part, wo_part, pos_copy, g_copy = copies(
        (x_hbm, pos_hbm, g_hbm, wq_hbm, wk_hbm, wv_hbm, wo_hbm, out_v, pos_v, g_v, wkv_v, wq_v, x_sem, small_sem, first_sem, wkv_sem, wq_sem))

    g_copy.start()
    for i in range(X_PARTS):
        x_part(i).start()
    pos_copy.start()
    for t in range(SLICES // 2):
        for copy in wkv_slice(t):
            copy.start()
    barrier = pltpu.get_barrier_semaphore()
    for t in range(2):
        for c in range(4):
            @pl.when((tp != t) | (cp != c))
            def _():
                pl.semaphore_signal(barrier, inc=1, device_id={"tp": t, "cp": c}, device_id_type=MESH)

    def normalise(i):
        rows = pl.ds(i * X_ROWS, X_ROWS)
        inv = inv_v[rows, :]
        for t in range(WIDTH // HEAD):
            lanes = pl.ds(t * HEAD, HEAD)
            h_v[rows, lanes] = (out_v[rows, lanes].astype(F32) * inv * gain_v[pl.ds(t, 1), :]).astype(BF16)

    g_copy.wait()
    gain_v[...] = g_v[...].astype(F32)
    for i in range(X_PARTS):
        x_part(i).wait()
        if i == 0:
            for t in range(SLICES // 2, SLICES):
                for copy in wkv_slice(t):
                    copy.start()
        if i == 3:
            for copy in wkv_rest:
                copy.start()
        rows = pl.ds(i * X_ROWS, X_ROWS)
        squares = None
        for t in range(WIDTH // HEAD):
            xf = out_v[rows, pl.ds(t * HEAD, HEAD)].astype(F32)
            squares = xf * xf if squares is None else squares + xf * xf
        mean = jnp.sum(squares, axis=-1, keepdims=True) * (1.0 / WIDTH)
        if i:
            normalise(i - 1)
        inv_v[rows, :] = jnp.broadcast_to(lax.rsqrt(mean + EPS), (X_ROWS, HEAD))
    normalise(X_PARTS - 1)

    def piece(block, h):
        return kv_v.at[h, pl.ds(pl.multiple_of(block * ROWS, ROWS), ROWS), :]

    def kv_copy(src_block, h, target):
        return pltpu.make_async_remote_copy(
            src_ref=piece(src_block, h), dst_ref=piece(src_block, h), send_sem=kv_send,
            recv_sem=kv_recv.at[src_block, h], device_id={"cp": target}, device_id_type=MESH)

    def heads_of(acc, pair):
        for a in range(2):
            h = 2 * pair + a
            k = rope(acc[:, a * HEAD:(a + 1) * HEAD], cos_v[...], sin_v[...]).astype(BF16)
            piece(cp, h)[:, pl.ds(0, HEAD)] = k
            piece(cp, h)[:, pl.ds(HEAD, HEAD)] = acc[:, PAIR + a * HEAD:PAIR + (a + 1) * HEAD].astype(BF16)

    def send_heads(pair):
        for h in (2 * pair, 2 * pair + 1):
            @pl.when(cp == 0)
            def _():
                kv_copy(0, h, 2).start()
                kv_copy(0, h, 1).start()

            @pl.when(cp == 1)
            def _():
                kv_copy(1, h, 3).start()

            @pl.when(cp == 2)
            def _():
                kv_copy(2, h, 3).start()

    def query_heads(acc, j):
        for g in range(GROUP):
            q = rope(acc[:, g * HEAD:(g + 1) * HEAD], cos_v[...], sin_v[...]).astype(BF16)
            for half in range(2):
                q_v[j, pl.ds(half * QCOLS + g * HEAD, HEAD), :] = q[half * HEAD:(half + 1) * HEAD]

    pos_copy.wait()
    acc = None
    for part in range(4):
        for t in range(part * SLICES // 4, (part + 1) * SLICES // 4):
            wait_bytes(wkv_v.at[0, pl.ds(t * SLICE_ROWS, SLICE_ROWS), :], first_sem.at[t])
        if part == 0:
            wq_part(0).start()
        deep = pl.ds(part * WIDTH // 4, WIDTH // 4)
        d = jnp.dot(h_v[:, deep], wkv_v[0, deep, :], preferred_element_type=F32)
        acc = d if acc is None else acc + d
        if part == 0:
            rope_tables(pos_v, cos_v, sin_v)
    wq_part(1).start()
    heads_of(acc, 0)
    pl.semaphore_wait(barrier, 7)
    send_heads(0)

    wait_bytes(wkv_v.at[1], wkv_sem)
    wq_part(2).start()
    pending = jnp.dot(h_v[...], wkv_v[1], preferred_element_type=F32)

    def forward_to(block, h, target):
        kv_copy(block, h, target).wait_recv()
        kv_copy(block, h, target).start()

    def forward(h):
        @pl.when(cp == 2)
        def _():
            forward_to(0, h, 3)

        @pl.when(cp == 3)
        def _():
            forward_to(1, h, 2)

    stats = (q_v, kv_v, o_v, max_v, sum_v, acc_v, score_v, weight_v)
    for j in range(KV):
        wq_part(j).wait()
        if j == 0:
            wq_part(3).start()
        acc = jnp.dot(h_v[...], wq_v[j], preferred_element_type=F32)
        if j == 0:
            heads_of(pending, 1)
            send_heads(1)
        else:
            query_heads(pending, j - 1)
        pending = acc
        for copy in wo_part(j):
            copy.start()
        if j == KV - 1:
            forward(0)
    query_heads(pending, KV - 1)
    attend(own_units(pl.multiple_of(cp * ROWS, ROWS)), False, True, *stats)
    forward(1)

    def arrive(src_block, h):
        kv_copy(src_block, h, 0).wait_recv()

    @pl.when(cp == 1)
    def _():
        for h in range(KV):
            arrive(0, h)
        attend(block_units(range(KV), 0, 1), True, True, *stats)

    @pl.when(cp == 2)
    def _():
        arrive(1, 0)
        arrive(1, 1)
        attend(block_units((0, 1), 0, 2), True, True, *stats)
        forward_to(0, 2, 3)
        arrive(1, 2)
        attend(block_units((2,), 0, 2), True, True, *stats)
        forward_to(0, 3, 3)
        arrive(1, 3)
        attend(block_units((3,), 0, 2), True, True, *stats)

    @pl.when(cp == 3)
    def _():
        for h in range(KV):
            arrive(2, h)
        attend(block_units((0, 1), 2, 3), True, False, *stats)
        forward_to(1, 2, 2)
        attend(block_units((2, 3), 2, 3), True, False, *stats)
        arrive(0, 0)
        attend(block_units((0,), 0, 2), True, True, *stats)
        forward_to(1, 3, 2)
        arrive(0, 1)
        arrive(0, 2)
        attend(block_units((1, 2), 0, 2), True, True, *stats)
        arrive(0, 3)
        attend(block_units((3,), 0, 2), True, True, *stats)

    def sent(n):
        return wkv_v.at[0, pl.ds(pl.multiple_of(n * ROWS, ROWS), ROWS), pl.ds(0, OCHUNK)]

    def group(n):
        early = (n + 1) // 4
        return jnp.where(n < 14, early, n - 10) if not isinstance(n, int) else (early if n < 14 else n - 10)

    def p_copy(n):
        return pltpu.make_async_remote_copy(
            src_ref=sent(n), dst_ref=precv.at[n], send_sem=p_send, recv_sem=p_recv.at[group(n)],
            device_id={"tp": other}, device_id_type=MESH)

    def held(me, i):
        return pl.ds(sum(DETOUR_ROWS[me][:i]), DETOUR_ROWS[me][i])

    def relay_in(me, i):
        return pltpu.make_async_remote_copy(
            src_ref=sent(i).at[pl.ds(0, DETOUR_ROWS[me][i])], dst_ref=relay_v.at[held(me, i)], send_sem=p_send, recv_sem=relay_recv,
            device_id={"tp": other, "cp": 4 - me}, device_id_type=MESH)

    def relay_out(me, i):
        return pltpu.make_async_remote_copy(
            src_ref=relay_v.at[held(me, i)], dst_ref=precv.at[i, pl.ds(0, DETOUR_ROWS[me][i])], send_sem=relay_send, recv_sem=p_recv.at[group(i)],
            device_id={"cp": me}, device_id_type=MESH)

    def rest(me, i):
        rows = pl.ds(DETOUR_ROWS[me][i], ROWS - DETOUR_ROWS[me][i])
        return pltpu.make_async_remote_copy(
            src_ref=sent(i).at[rows], dst_ref=precv.at[i, rows], send_sem=p_send, recv_sem=p_recv.at[group(i)],
            device_id={"tp": other}, device_id_type=MESH)

    def pass_on(me):
        wait_bytes(relay_v.at[pl.ds(0, sum(DETOUR_ROWS[me]))], relay_recv)
        for i in range(len(DETOUR_ROWS[me])):
            relay_out(me, i).start()

    def passed_on(me):
        wait_bytes(relay_v.at[pl.ds(0, sum(DETOUR_ROWS[me]))], relay_send)

    @pl.loop(0, NOUT)
    def _(n):
        @pl.when(lax.rem(n, 4) == 0)
        def _():
            wait_bytes(wq_v.at[n // 4], wq_sem.at[n // 4])

        room = wo_room(wq_v, n)
        part = None
        for h in range(KV):
            d = jnp.dot(o_v[h], room[pl.ds(h * QCOLS, QCOLS), :], preferred_element_type=F32)
            part = d if part is None else part + d
        sent(n)[...] = part.astype(BF16)
        for me, detours in DETOUR_ROWS.items():
            for i in range(len(detours)):
                @pl.when((cp == me) & (n == i))
                def _():
                    relay_in(me, i).start()
                    if detours[i] < ROWS:
                        rest(me, i).start()

        direct = lax.rem(cp, 2) == 0
        for me, detours in DETOUR_ROWS.items():
            direct = direct | ((cp == me) & (n >= len(detours)))

        @pl.when(direct)
        def _():
            p_copy(n).start()

    @pl.when(cp == 3)
    def _():
        pass_on(1)

    for cache, lanes in ((k_out, pl.ds(0, HEAD)), (v_out, pl.ds(HEAD, HEAD))):
        for h in range(KV):
            cache_v[pl.ds(h, ROWS, stride=KV), :] = piece(cp, h)[:, lanes].astype(F32)
        cache[...] = cache_v[...].astype(BF16)

    @pl.when(lax.rem(cp, 2) == 0)
    def _():
        wait_bytes(kv_v.at[:, pl.ds(0, 2 * ROWS), :], kv_send)

    @pl.when(lax.rem(cp, 2) == 1)
    def _():
        wait_bytes(kv_v.at[:, pl.ds(0, ROWS), :], kv_send)

    def add_chunks(first, count):
        wait_bytes(precv.at[pl.ds(first, count)], p_recv.at[group(first)])
        for n in range(first, first + count):
            cols = pl.ds(n * OCHUNK, OCHUNK)
            total = sent(n)[...].astype(F32) + precv[n].astype(F32)
            out_v[:, cols] = (out_v[:, cols].astype(F32) + total).astype(BF16)

    add_chunks(3, 4)
    add_chunks(7, 4)

    @pl.when(cp == 1)
    def _():
        pass_on(3)

    @pl.when(cp == 3)
    def _():
        passed_on(1)

    add_chunks(11, 3)

    @pl.when(cp == 1)
    def _():
        passed_on(3)

    add_chunks(0, 3)
    add_chunks(14, 1)
    add_chunks(15, 1)
    wait_bytes(precv, p_send)


def store_results(out_v, k_v, v_v, out_hbm, k_hbm, v_hbm, sem):
    stores = [pltpu.make_async_copy(src, dst, sem.at[i]) for i, (src, dst) in enumerate(((out_v, out_hbm), (k_v, k_hbm), (v_v, v_hbm)))]
    for store in stores:
        store.start()
    for store in stores:
        store.wait()


def solution(mesh):
    row_spec = P(('dp', 'cp'), None)
    cache_spec = P(('dp', 'cp'), 'tp', None)
    head_cols = P(None, 'tp')

    def local_block(hidden, positions, norm_gain, w_query, w_key, w_value, w_out):
        dma = pltpu.SemaphoreType.DMA
        out, k_rope, v_heads = pl.pallas_call(
            kernel,
            out_shape=[
                jax.ShapeDtypeStruct((ROWS, WIDTH), BF16),
                jax.ShapeDtypeStruct((ROWS * KV, HEAD), BF16),
                jax.ShapeDtypeStruct((ROWS * KV, HEAD), BF16),
            ],
            in_specs=[pl.BlockSpec(memory_space=pltpu.HBM)] * 7,
            out_specs=[pl.BlockSpec(memory_space=pltpu.VMEM)] * 3,
            scratch_shapes=[
                pltpu.VMEM((ROWS,), jnp.int32),
                pltpu.VMEM((WIDTH // HEAD, HEAD), BF16),
                pltpu.VMEM((2, WIDTH, 2 * PAIR), BF16),
                pltpu.VMEM((KV, WIDTH, QCOLS), BF16),
                pltpu.VMEM((ROWS, WIDTH), BF16),
                pltpu.VMEM((WIDTH // HEAD, HEAD), F32),
                pltpu.VMEM((ROWS, HEAD), F32),
                pltpu.VMEM((ROWS, HEAD), F32),
                pltpu.VMEM((ROWS, HEAD), F32),
                pltpu.VMEM((KV, 4 * ROWS, 2 * HEAD), BF16),
                pltpu.VMEM((KV, GROUP * ROWS, HEAD), BF16),
                pltpu.VMEM((KV, ROWS, QCOLS), BF16),
                pltpu.VMEM((KV, 1, GROUP * ROWS), F32),
                pltpu.VMEM((KV, 1, GROUP * ROWS), F32),
                pltpu.VMEM((KV, HEAD, GROUP * ROWS), F32),
                pltpu.VMEM((KV * ROWS, GROUP * ROWS), F32),
                pltpu.VMEM((KV * ROWS, GROUP * ROWS), BF16),
                pltpu.VMEM((NOUT, ROWS, OCHUNK), BF16),
                pltpu.VMEM((max(map(sum, DETOUR_ROWS.values())), OCHUNK), BF16),
                pltpu.VMEM((ROWS * KV, HEAD), F32),
                dma((X_PARTS,)), dma((2,)), dma((SLICES,)), dma, dma((KV,)),
                dma, dma((3, KV)), dma, dma((6,)), dma, dma,
            ],
            compiler_params=pltpu.CompilerParams(collective_id=0, has_side_effects=True, vmem_limit_bytes=49 << 20),
        )(*(pltpu.with_memory_space_constraint(a, pltpu.HBM) for a in (hidden, positions, norm_gain.reshape(WIDTH // HEAD, HEAD), w_query, w_key, w_value, w_out)))
        out, k_rope, v_heads = pl.pallas_call(
            store_results,
            out_shape=[jax.ShapeDtypeStruct(a.shape, BF16) for a in (out, k_rope, v_heads)],
            in_specs=[pl.BlockSpec(memory_space=pltpu.VMEM)] * 3,
            out_specs=[pl.BlockSpec(memory_space=pl.ANY)] * 3,
            scratch_shapes=[dma((3,))],
            compiler_params=pltpu.CompilerParams(vmem_limit_bytes=4 << 20),
        )(out, k_rope, v_heads)
        return out, k_rope.reshape(ROWS, KV, HEAD), v_heads.reshape(ROWS, KV, HEAD)

    return jax.shard_map(local_block, mesh=mesh, in_specs=(row_spec, P(('dp', 'cp')), P(None), head_cols, head_cols, head_cols, P('tp', None)), out_specs=(row_spec, cache_spec, cache_spec), check_vma=False)
```

```python
import functools
import math

import jax
import jax.numpy as jnp
from jax import lax
from jax.experimental import pallas as pl
from jax.experimental.pallas import tpu as pltpu
from jax.sharding import PartitionSpec as P

HEAD = 128
HALF = HEAD // 2
EPS = 1e-5
LOG_THETA = math.log(1000000.0)
SCORE_SCALE = 1.0 / math.sqrt(HEAD)
EXP2_SCALE = SCORE_SCALE / math.log(2.0)
MESH = pl.DeviceIdType.MESH
ROWS = 256
WIDTH = 4096
KV = 4
GROUP = 4
QCOLS = GROUP * HEAD
PAIR = 2 * HEAD
OCHUNK = 256
NOUT = WIDTH // OCHUNK
X_PARTS = 4
X_ROWS = ROWS // X_PARTS
SLICE_ROWS = 1024
SLICES = WIDTH // SLICE_ROWS
KEY_ROWS = 32
DETOUR_ROWS = {1: (256, 256, 256), 3: (256, 256, 192)}
F32 = jnp.float32
BF16 = jnp.bfloat16


def wo_room(wq_v, n):
    deep = KV * QCOLS
    row = pl.multiple_of(lax.rem(n, 4) // 2 * deep, deep)
    col = pl.multiple_of(lax.rem(n, 2) * OCHUNK, OCHUNK)
    return wq_v.at[n // 4, pl.ds(row, deep), pl.ds(col, OCHUNK)]


def wait_bytes(room, sem):
    pltpu.make_async_copy(room, room, sem).wait()


def copies(refs):
    (x_hbm, pos_hbm, g_hbm, wq_hbm, wk_hbm, wv_hbm, wo_hbm, x_v, pos_v, g_v, wkv_v, wq_v, x_sem, small_sem, first_sem, wkv_sem, wq_sem) = refs

    def x_part(i):
        return pltpu.make_async_copy(x_hbm.at[pl.ds(i * X_ROWS, X_ROWS)], x_v.at[pl.ds(i * X_ROWS, X_ROWS)], x_sem.at[i])

    def wkv_slice(t):
        rows = pl.ds(t * SLICE_ROWS, SLICE_ROWS)
        return [pltpu.make_async_copy(w.at[rows, pl.ds(0, PAIR)], wkv_v.at[0, rows, pl.ds(a * PAIR, PAIR)], first_sem.at[t]) for a, w in enumerate((wk_hbm, wv_hbm))]

    wkv_rest = [pltpu.make_async_copy(w.at[:, pl.ds(PAIR, PAIR)], wkv_v.at[1, :, pl.ds(a * PAIR, PAIR)], wkv_sem) for a, w in enumerate((wk_hbm, wv_hbm))]

    def wq_part(j):
        return pltpu.make_async_copy(wq_hbm.at[:, pl.ds(j * QCOLS, QCOLS)], wq_v.at[j], wq_sem.at[j])

    def wo_part(j):
        deep = KV * QCOLS
        parts = []
        for a in range(2):
            cols = pl.ds(pl.multiple_of((2 * j + a) * QCOLS, QCOLS), QCOLS)
            parts.append(pltpu.make_async_copy(wo_hbm.at[:, cols], wq_v.at[j, pl.ds(a * deep, deep), :], wq_sem.at[j]))
        return parts

    pos_copy = pltpu.make_async_copy(pos_hbm, pos_v, small_sem.at[0])
    g_copy = pltpu.make_async_copy(g_hbm, g_v, small_sem.at[1])
    return x_part, wkv_slice, wkv_rest, wq_part, wo_part, pos_copy, g_copy


def rope_tables(pos_v, cos_v, sin_v):
    lane = lax.broadcasted_iota(jnp.int32, (1, HEAD), 1)
    inv_freq = jnp.exp(lax.rem(lane, HALF).astype(F32) * (-2.0 * LOG_THETA / HEAD))
    low = lane < HALF
    top = jnp.broadcast_to(pos_v[pl.ds(0, HEAD)].reshape(1, HEAD).astype(F32), (HEAD, HEAD)).T
    bottom = jnp.broadcast_to(pos_v[pl.ds(HEAD, HEAD)].reshape(1, HEAD).astype(F32), (HEAD, HEAD)).T
    angles = jnp.where(low, top, bottom) * inv_freq
    cos_t, sin_t = jnp.cos(angles), jnp.sin(angles)
    cos_r, sin_r = pltpu.roll(cos_t, HALF, 1), pltpu.roll(sin_t, HALF, 1)
    cos_v[pl.ds(0, HEAD)] = jnp.where(low, cos_t, cos_r)
    cos_v[pl.ds(HEAD, HEAD)] = jnp.where(low, cos_r, cos_t)
    sin_v[pl.ds(0, HEAD)] = jnp.where(low, -sin_t, sin_r)
    sin_v[pl.ds(HEAD, HEAD)] = jnp.where(low, -sin_r, sin_t)


def rope(vals, cos_t, sin_t):
    return vals * cos_t + pltpu.roll(vals, HALF, 1) * sin_t


def attend(units, merge, last, q_v, kv_v, o_v, max_v, sum_v, acc_v, score_v, weight_v):
    tops, sums = {}, {}

    def room(h, count):
        return h * ROWS if count <= ROWS else h % 2 * 2 * ROWS

    def score_phase(unit):
        h, start, count, first, width, causal = unit
        lanes = pl.ds(first, width)
        s = lax.dot_general(kv_v[h, pl.ds(start, count), pl.ds(0, HEAD)], q_v[h, lanes, :], (((1,), (1,)), ((), ())), preferred_element_type=F32)
        parts = [(0, s)]
        if causal:
            key = lax.broadcasted_iota(jnp.int32, (HEAD, width), 0)
            query = lax.rem(lax.broadcasted_iota(jnp.int32, (HEAD, width), 1), HEAD)
            free = count - HEAD
            parts = ([(0, s[:free])] if free else []) + [(free, jnp.where(key <= query, s[free:], -jnp.inf))]
        tall = []
        for row, part in parts:
            score_v[pl.ds(room(h, count) + row, part.shape[0]), lanes] = part
            tall.append(jnp.max(part.reshape(part.shape[0] // 8, 8, width), axis=0))
        top = jnp.max(functools.reduce(jnp.maximum, tall), axis=0, keepdims=True) * EXP2_SCALE
        tops[h, first] = jnp.maximum(top, max_v[h, :, lanes]) if merge else top

    def weight_phase(unit):
        h, start, count, first, width, causal = unit
        lanes = pl.ds(first, width)
        total = None
        for c in range(count // KEY_ROWS):
            rows = pl.ds(room(h, count) + c * KEY_ROWS, KEY_ROWS)
            w = jnp.exp2(score_v[rows, lanes] * EXP2_SCALE - tops[h, first])
            part = jnp.sum(w.reshape(KEY_ROWS // 8, 8, width), axis=0)
            total = part if total is None else total + part
            weight_v[rows, lanes] = w.astype(BF16)
        sums[h, first] = total

    def value_phase(unit):
        h, start, count, first, width, causal = unit
        lanes = pl.ds(first, width)
        acc = lax.dot_general(kv_v[h, pl.ds(start, count), pl.ds(HEAD, HEAD)], weight_v[pl.ds(room(h, count), count), lanes], (((0,), (0,)), ((), ())), preferred_element_type=F32)
        total = jnp.sum(sums[h, first], axis=0, keepdims=True)
        if merge:
            scale = jnp.exp2(max_v[h, :, lanes] - tops[h, first])
            total, acc = sum_v[h, :, lanes] * scale + total, acc_v[h, :, lanes] * scale + acc
        if not (merge and last):
            max_v[h, :, lanes], sum_v[h, :, lanes], acc_v[h, :, lanes] = tops[h, first], total, acc
        if last:
            vals = (acc / total).astype(BF16)
            for i in range(width // HEAD):
                half, g = divmod(first // HEAD + i, GROUP)
                o_v[h, pl.ds(half * HEAD, HEAD), pl.ds(g * HEAD, HEAD)] = vals[:, i * HEAD:(i + 1) * HEAD].T

    for i in range(len(units) + 2):
        if i < len(units):
            score_phase(units[i])
        if 0 <= i - 1 < len(units):
            weight_phase(units[i - 1])
        if 0 <= i - 2 < len(units):
            value_phase(units[i - 2])


def own_units(start):
    return [(h, start, (half + 1) * HEAD, half * QCOLS, QCOLS, True) for h in range(KV) for half in range(2)]


def block_units(heads, first, end):
    return [(h, first * ROWS, (end - first) * ROWS, 0, GROUP * ROWS, False) for h in heads]


def kernel(x_hbm, pos_hbm, g_hbm, wq_hbm, wk_hbm, wv_hbm, wo_hbm,
           out_v, k_out, v_out,
           pos_v, g_v, wkv_v, wq_v, h_v, gain_v, inv_v, cos_v, sin_v, kv_v, q_v, o_v, max_v, sum_v, acc_v, score_v, weight_v, precv, relay_v, cache_v,
           x_sem, small_sem, first_sem, wkv_sem, wq_sem, kv_send, kv_recv, p_send, p_recv, relay_send, relay_recv):
    tp, cp = lax.axis_index("tp"), lax.axis_index("cp")
    other = 1 - tp
    x_part, wkv_slice, wkv_rest, wq_part, wo_part, pos_copy, g_copy = copies(
        (x_hbm, pos_hbm, g_hbm, wq_hbm, wk_hbm, wv_hbm, wo_hbm, out_v, pos_v, g_v, wkv_v, wq_v, x_sem, small_sem, first_sem, wkv_sem, wq_sem))

    g_copy.start()
    for i in range(X_PARTS):
        x_part(i).start()
    pos_copy.start()
    for t in range(1):
        for copy in wkv_slice(t):
            copy.start()
    barrier = pltpu.get_barrier_semaphore()
    for t in range(2):
        for c in range(4):
            @pl.when((tp != t) | (cp != c))
            def _():
                pl.semaphore_signal(barrier, inc=1, device_id={"tp": t, "cp": c}, device_id_type=MESH)

    def normalise(i):
        rows = pl.ds(i * X_ROWS, X_ROWS)
        inv = inv_v[rows, :]
        for t in range(WIDTH // HEAD):
            lanes = pl.ds(t * HEAD, HEAD)
            h_v[rows, lanes] = (out_v[rows, lanes].astype(F32) * inv * gain_v[pl.ds(t, 1), :]).astype(BF16)

    g_copy.wait()
    gain_v[...] = g_v[...].astype(F32)
    for i in range(X_PARTS):
        x_part(i).wait()
        if i == 0:
            for t in range(1, SLICES):
                for copy in wkv_slice(t):
                    copy.start()
        if i == 3:
            for copy in wkv_rest:
                copy.start()
        rows = pl.ds(i * X_ROWS, X_ROWS)
        squares = None
        for t in range(WIDTH // HEAD):
            xf = out_v[rows, pl.ds(t * HEAD, HEAD)].astype(F32)
            squares = xf * xf if squares is None else squares + xf * xf
        mean = jnp.sum(squares, axis=-1, keepdims=True) * (1.0 / WIDTH)
        if i:
            normalise(i - 1)
        inv_v[rows, :] = jnp.broadcast_to(lax.rsqrt(mean + EPS), (X_ROWS, HEAD))
    normalise(X_PARTS - 1)

    def piece(block, h):
        return kv_v.at[h, pl.ds(pl.multiple_of(block * ROWS, ROWS), ROWS), :]

    def kv_copy(src_block, h, target):
        return pltpu.make_async_remote_copy(
            src_ref=piece(src_block, h), dst_ref=piece(src_block, h), send_sem=kv_send,
            recv_sem=kv_recv.at[src_block, h], device_id={"cp": target}, device_id_type=MESH)

    def heads_of(acc, pair):
        for a in range(2):
            h = 2 * pair + a
            k = rope(acc[:, a * HEAD:(a + 1) * HEAD], cos_v[...], sin_v[...]).astype(BF16)
            piece(cp, h)[:, pl.ds(0, HEAD)] = k
            piece(cp, h)[:, pl.ds(HEAD, HEAD)] = acc[:, PAIR + a * HEAD:PAIR + (a + 1) * HEAD].astype(BF16)

    def send_heads(pair):
        for h in (2 * pair, 2 * pair + 1):
            @pl.when(cp == 0)
            def _():
                kv_copy(0, h, 2).start()
                kv_copy(0, h, 1).start()

            @pl.when(cp == 1)
            def _():
                kv_copy(1, h, 3).start()

            @pl.when(cp == 2)
            def _():
                kv_copy(2, h, 3).start()

    def query_heads(acc, j):
        for g in range(GROUP):
            q = rope(acc[:, g * HEAD:(g + 1) * HEAD], cos_v[...], sin_v[...]).astype(BF16)
            for half in range(2):
                q_v[j, pl.ds(half * QCOLS + g * HEAD, HEAD), :] = q[half * HEAD:(half + 1) * HEAD]

    pos_copy.wait()
    acc = None
    for part in range(4):
        for t in range(part * SLICES // 4, (part + 1) * SLICES // 4):
            wait_bytes(wkv_v.at[0, pl.ds(t * SLICE_ROWS, SLICE_ROWS), :], first_sem.at[t])
        if part == 0:
            wq_part(0).start()
        deep = pl.ds(part * WIDTH // 4, WIDTH // 4)
        d = jnp.dot(h_v[:, deep], wkv_v[0, deep, :], preferred_element_type=F32)
        acc = d if acc is None else acc + d
        if part == 0:
            rope_tables(pos_v, cos_v, sin_v)
    wq_part(1).start()
    heads_of(acc, 0)
    pl.semaphore_wait(barrier, 7)
    send_heads(0)

    wait_bytes(wkv_v.at[1], wkv_sem)
    wq_part(2).start()
    pending = jnp.dot(h_v[...], wkv_v[1], preferred_element_type=F32)

    def forward_to(block, h, target):
        kv_copy(block, h, target).wait_recv()
        kv_copy(block, h, target).start()

    def forward(h):
        @pl.when(cp == 2)
        def _():
            forward_to(0, h, 3)

        @pl.when(cp == 3)
        def _():
            forward_to(1, h, 2)

    stats = (q_v, kv_v, o_v, max_v, sum_v, acc_v, score_v, weight_v)
    for j in range(KV):
        wq_part(j).wait()
        if j == 0:
            wq_part(3).start()
        acc = jnp.dot(h_v[...], wq_v[j], preferred_element_type=F32)
        if j == 0:
            heads_of(pending, 1)
            send_heads(1)
        else:
            query_heads(pending, j - 1)
        pending = acc
        for copy in wo_part(j):
            copy.start()
        if j == KV - 1:
            forward(0)
    query_heads(pending, KV - 1)
    attend(own_units(pl.multiple_of(cp * ROWS, ROWS)), False, True, *stats)
    forward(1)

    def arrive(src_block, h):
        kv_copy(src_block, h, 0).wait_recv()

    @pl.when(cp == 1)
    def _():
        for h in range(KV):
            arrive(0, h)
        attend(block_units(range(KV), 0, 1), True, True, *stats)

    @pl.when(cp == 2)
    def _():
        arrive(1, 0)
        arrive(1, 1)
        attend(block_units((0, 1), 0, 2), True, True, *stats)
        forward_to(0, 2, 3)
        arrive(1, 2)
        attend(block_units((2,), 0, 2), True, True, *stats)
        forward_to(0, 3, 3)
        arrive(1, 3)
        attend(block_units((3,), 0, 2), True, True, *stats)

    @pl.when(cp == 3)
    def _():
        for h in range(KV):
            arrive(2, h)
        attend(block_units((0, 1), 2, 3), True, False, *stats)
        forward_to(1, 2, 2)
        attend(block_units((2, 3), 2, 3), True, False, *stats)
        arrive(0, 0)
        attend(block_units((0,), 0, 2), True, True, *stats)
        forward_to(1, 3, 2)
        arrive(0, 1)
        arrive(0, 2)
        attend(block_units((1, 2), 0, 2), True, True, *stats)
        arrive(0, 3)
        attend(block_units((3,), 0, 2), True, True, *stats)

    def sent(n):
        return wkv_v.at[0, pl.ds(pl.multiple_of(n * ROWS, ROWS), ROWS), pl.ds(0, OCHUNK)]

    def group(n):
        early = (n + 1) // 4
        return jnp.where(n < 14, early, n - 10) if not isinstance(n, int) else (early if n < 14 else n - 10)

    def p_copy(n):
        return pltpu.make_async_remote_copy(
            src_ref=sent(n), dst_ref=precv.at[n], send_sem=p_send, recv_sem=p_recv.at[group(n)],
            device_id={"tp": other}, device_id_type=MESH)

    def held(me, i):
        return pl.ds(sum(DETOUR_ROWS[me][:i]), DETOUR_ROWS[me][i])

    def relay_in(me, i):
        return pltpu.make_async_remote_copy(
            src_ref=sent(i).at[pl.ds(0, DETOUR_ROWS[me][i])], dst_ref=relay_v.at[held(me, i)], send_sem=p_send, recv_sem=relay_recv,
            device_id={"tp": other, "cp": 4 - me}, device_id_type=MESH)

    def relay_out(me, i):
        return pltpu.make_async_remote_copy(
            src_ref=relay_v.at[held(me, i)], dst_ref=precv.at[i, pl.ds(0, DETOUR_ROWS[me][i])], send_sem=relay_send, recv_sem=p_recv.at[group(i)],
            device_id={"cp": me}, device_id_type=MESH)

    def rest(me, i):
        rows = pl.ds(DETOUR_ROWS[me][i], ROWS - DETOUR_ROWS[me][i])
        return pltpu.make_async_remote_copy(
            src_ref=sent(i).at[rows], dst_ref=precv.at[i, rows], send_sem=p_send, recv_sem=p_recv.at[group(i)],
            device_id={"tp": other}, device_id_type=MESH)

    def pass_on(me):
        wait_bytes(relay_v.at[pl.ds(0, sum(DETOUR_ROWS[me]))], relay_recv)
        for i in range(len(DETOUR_ROWS[me])):
            relay_out(me, i).start()

    def passed_on(me):
        wait_bytes(relay_v.at[pl.ds(0, sum(DETOUR_ROWS[me]))], relay_send)

    @pl.loop(0, NOUT)
    def _(n):
        @pl.when(lax.rem(n, 4) == 0)
        def _():
            wait_bytes(wq_v.at[n // 4], wq_sem.at[n // 4])

        room = wo_room(wq_v, n)
        part = None
        for h in range(KV):
            d = jnp.dot(o_v[h], room[pl.ds(h * QCOLS, QCOLS), :], preferred_element_type=F32)
            part = d if part is None else part + d
        sent(n)[...] = part.astype(BF16)
        for me, detours in DETOUR_ROWS.items():
            for i in range(len(detours)):
                @pl.when((cp == me) & (n == i))
                def _():
                    relay_in(me, i).start()
                    if detours[i] < ROWS:
                        rest(me, i).start()

        direct = lax.rem(cp, 2) == 0
        for me, detours in DETOUR_ROWS.items():
            direct = direct | ((cp == me) & (n >= len(detours)))

        @pl.when(direct)
        def _():
            p_copy(n).start()

    @pl.when(cp == 3)
    def _():
        pass_on(1)

    for cache, lanes in ((k_out, pl.ds(0, HEAD)), (v_out, pl.ds(HEAD, HEAD))):
        for h in range(KV):
            cache_v[pl.ds(h, ROWS, stride=KV), :] = piece(cp, h)[:, lanes].astype(F32)
        cache[...] = cache_v[...].astype(BF16)

    @pl.when(lax.rem(cp, 2) == 0)
    def _():
        wait_bytes(kv_v.at[:, pl.ds(0, 2 * ROWS), :], kv_send)

    @pl.when(lax.rem(cp, 2) == 1)
    def _():
        wait_bytes(kv_v.at[:, pl.ds(0, ROWS), :], kv_send)

    def add_chunks(first, count):
        wait_bytes(precv.at[pl.ds(first, count)], p_recv.at[group(first)])
        for n in range(first, first + count):
            cols = pl.ds(n * OCHUNK, OCHUNK)
            total = sent(n)[...].astype(F32) + precv[n].astype(F32)
            out_v[:, cols] = (out_v[:, cols].astype(F32) + total).astype(BF16)

    add_chunks(3, 4)
    add_chunks(7, 4)

    @pl.when(cp == 1)
    def _():
        pass_on(3)

    @pl.when(cp == 3)
    def _():
        passed_on(1)

    add_chunks(11, 3)

    @pl.when(cp == 1)
    def _():
        passed_on(3)

    add_chunks(0, 3)
    add_chunks(14, 1)
    add_chunks(15, 1)
    wait_bytes(precv, p_send)


def store_results(out_v, k_v, v_v, out_hbm, k_hbm, v_hbm, sem):
    stores = [pltpu.make_async_copy(src, dst, sem.at[i]) for i, (src, dst) in enumerate(((out_v, out_hbm), (k_v, k_hbm), (v_v, v_hbm)))]
    for store in stores:
        store.start()
    for store in stores:
        store.wait()


def solution(mesh):
    row_spec = P(('dp', 'cp'), None)
    cache_spec = P(('dp', 'cp'), 'tp', None)
    head_cols = P(None, 'tp')

    def local_block(hidden, positions, norm_gain, w_query, w_key, w_value, w_out):
        dma = pltpu.SemaphoreType.DMA
        out, k_rope, v_heads = pl.pallas_call(
            kernel,
            out_shape=[
                jax.ShapeDtypeStruct((ROWS, WIDTH), BF16),
                jax.ShapeDtypeStruct((ROWS * KV, HEAD), BF16),
                jax.ShapeDtypeStruct((ROWS * KV, HEAD), BF16),
            ],
            in_specs=[pl.BlockSpec(memory_space=pltpu.HBM)] * 7,
            out_specs=[pl.BlockSpec(memory_space=pltpu.VMEM)] * 3,
            scratch_shapes=[
                pltpu.VMEM((ROWS,), jnp.int32),
                pltpu.VMEM((WIDTH // HEAD, HEAD), BF16),
                pltpu.VMEM((2, WIDTH, 2 * PAIR), BF16),
                pltpu.VMEM((KV, WIDTH, QCOLS), BF16),
                pltpu.VMEM((ROWS, WIDTH), BF16),
                pltpu.VMEM((WIDTH // HEAD, HEAD), F32),
                pltpu.VMEM((ROWS, HEAD), F32),
                pltpu.VMEM((ROWS, HEAD), F32),
                pltpu.VMEM((ROWS, HEAD), F32),
                pltpu.VMEM((KV, 4 * ROWS, 2 * HEAD), BF16),
                pltpu.VMEM((KV, GROUP * ROWS, HEAD), BF16),
                pltpu.VMEM((KV, ROWS, QCOLS), BF16),
                pltpu.VMEM((KV, 1, GROUP * ROWS), F32),
                pltpu.VMEM((KV, 1, GROUP * ROWS), F32),
                pltpu.VMEM((KV, HEAD, GROUP * ROWS), F32),
                pltpu.VMEM((KV * ROWS, GROUP * ROWS), F32),
                pltpu.VMEM((KV * ROWS, GROUP * ROWS), BF16),
                pltpu.VMEM((NOUT, ROWS, OCHUNK), BF16),
                pltpu.VMEM((max(map(sum, DETOUR_ROWS.values())), OCHUNK), BF16),
                pltpu.VMEM((ROWS * KV, HEAD), F32),
                dma((X_PARTS,)), dma((2,)), dma((SLICES,)), dma, dma((KV,)),
                dma, dma((3, KV)), dma, dma((6,)), dma, dma,
            ],
            compiler_params=pltpu.CompilerParams(collective_id=0, has_side_effects=True, vmem_limit_bytes=49 << 20),
        )(*(pltpu.with_memory_space_constraint(a, pltpu.HBM) for a in (hidden, positions, norm_gain.reshape(WIDTH // HEAD, HEAD), w_query, w_key, w_value, w_out)))
        out, k_rope, v_heads = pl.pallas_call(
            store_results,
            out_shape=[jax.ShapeDtypeStruct(a.shape, BF16) for a in (out, k_rope, v_heads)],
            in_specs=[pl.BlockSpec(memory_space=pltpu.VMEM)] * 3,
            out_specs=[pl.BlockSpec(memory_space=pl.ANY)] * 3,
            scratch_shapes=[dma((3,))],
            compiler_params=pltpu.CompilerParams(vmem_limit_bytes=4 << 20),
        )(out, k_rope, v_heads)
        return out, k_rope.reshape(ROWS, KV, HEAD), v_heads.reshape(ROWS, KV, HEAD)

    return jax.shard_map(local_block, mesh=mesh, in_specs=(row_spec, P(('dp', 'cp')), P(None), head_cols, head_cols, head_cols, P('tp', None)), out_specs=(row_spec, cache_spec, cache_spec), check_vma=False)
```

```python
import functools
import math

import jax
import jax.numpy as jnp
from jax import lax
from jax.experimental import pallas as pl
from jax.experimental.pallas import tpu as pltpu
from jax.sharding import PartitionSpec as P

HEAD = 128
HALF = HEAD // 2
EPS = 1e-5
LOG_THETA = math.log(1000000.0)
SCORE_SCALE = 1.0 / math.sqrt(HEAD)
EXP2_SCALE = SCORE_SCALE / math.log(2.0)
MESH = pl.DeviceIdType.MESH
ROWS = 256
WIDTH = 4096
KV = 4
GROUP = 4
QCOLS = GROUP * HEAD
PAIR = 2 * HEAD
OCHUNK = 256
NOUT = WIDTH // OCHUNK
X_PARTS = 4
X_ROWS = ROWS // X_PARTS
SLICE_ROWS = 1024
SLICES = WIDTH // SLICE_ROWS
KEY_ROWS = 32
DETOUR_ROWS = {1: (256, 256, 256), 3: (256, 256, 208)}
F32 = jnp.float32
BF16 = jnp.bfloat16


def wo_room(wq_v, n):
    deep = KV * QCOLS
    row = pl.multiple_of(lax.rem(n, 4) // 2 * deep, deep)
    col = pl.multiple_of(lax.rem(n, 2) * OCHUNK, OCHUNK)
    return wq_v.at[n // 4, pl.ds(row, deep), pl.ds(col, OCHUNK)]


def wait_bytes(room, sem):
    pltpu.make_async_copy(room, room, sem).wait()


def copies(refs):
    (x_hbm, pos_hbm, g_hbm, wq_hbm, wk_hbm, wv_hbm, wo_hbm, x_v, pos_v, g_v, wkv_v, wq_v, x_sem, small_sem, first_sem, wkv_sem, wq_sem) = refs

    def x_part(i):
        return pltpu.make_async_copy(x_hbm.at[pl.ds(i * X_ROWS, X_ROWS)], x_v.at[pl.ds(i * X_ROWS, X_ROWS)], x_sem.at[i])

    def wkv_slice(t):
        rows = pl.ds(t * SLICE_ROWS, SLICE_ROWS)
        return [pltpu.make_async_copy(w.at[rows, pl.ds(0, PAIR)], wkv_v.at[0, rows, pl.ds(a * PAIR, PAIR)], first_sem.at[t]) for a, w in enumerate((wk_hbm, wv_hbm))]

    wkv_rest = [pltpu.make_async_copy(w.at[:, pl.ds(PAIR, PAIR)], wkv_v.at[1, :, pl.ds(a * PAIR, PAIR)], wkv_sem) for a, w in enumerate((wk_hbm, wv_hbm))]

    def wq_part(j):
        return pltpu.make_async_copy(wq_hbm.at[:, pl.ds(j * QCOLS, QCOLS)], wq_v.at[j], wq_sem.at[j])

    def wo_part(j):
        deep = KV * QCOLS
        parts = []
        for a in range(2):
            cols = pl.ds(pl.multiple_of((2 * j + a) * QCOLS, QCOLS), QCOLS)
            parts.append(pltpu.make_async_copy(wo_hbm.at[:, cols], wq_v.at[j, pl.ds(a * deep, deep), :], wq_sem.at[j]))
        return parts

    pos_copy = pltpu.make_async_copy(pos_hbm, pos_v, small_sem.at[0])
    g_copy = pltpu.make_async_copy(g_hbm, g_v, small_sem.at[1])
    return x_part, wkv_slice, wkv_rest, wq_part, wo_part, pos_copy, g_copy


def rope_tables(pos_v, cos_v, sin_v):
    lane = lax.broadcasted_iota(jnp.int32, (1, HEAD), 1)
    inv_freq = jnp.exp(lax.rem(lane, HALF).astype(F32) * (-2.0 * LOG_THETA / HEAD))
    low = lane < HALF
    top = jnp.broadcast_to(pos_v[pl.ds(0, HEAD)].reshape(1, HEAD).astype(F32), (HEAD, HEAD)).T
    bottom = jnp.broadcast_to(pos_v[pl.ds(HEAD, HEAD)].reshape(1, HEAD).astype(F32), (HEAD, HEAD)).T
    angles = jnp.where(low, top, bottom) * inv_freq
    cos_t, sin_t = jnp.cos(angles), jnp.sin(angles)
    cos_r, sin_r = pltpu.roll(cos_t, HALF, 1), pltpu.roll(sin_t, HALF, 1)
    cos_v[pl.ds(0, HEAD)] = jnp.where(low, cos_t, cos_r)
    cos_v[pl.ds(HEAD, HEAD)] = jnp.where(low, cos_r, cos_t)
    sin_v[pl.ds(0, HEAD)] = jnp.where(low, -sin_t, sin_r)
    sin_v[pl.ds(HEAD, HEAD)] = jnp.where(low, -sin_r, sin_t)


def rope(vals, cos_t, sin_t):
    return vals * cos_t + pltpu.roll(vals, HALF, 1) * sin_t


def attend(units, merge, last, q_v, kv_v, o_v, max_v, sum_v, acc_v, score_v, weight_v):
    tops, sums = {}, {}

    def room(h, count):
        return h * ROWS if count <= ROWS else h % 2 * 2 * ROWS

    def score_phase(unit):
        h, start, count, first, width, causal = unit
        lanes = pl.ds(first, width)
        s = lax.dot_general(kv_v[h, pl.ds(start, count), pl.ds(0, HEAD)], q_v[h, lanes, :], (((1,), (1,)), ((), ())), preferred_element_type=F32)
        parts = [(0, s)]
        if causal:
            key = lax.broadcasted_iota(jnp.int32, (HEAD, width), 0)
            query = lax.rem(lax.broadcasted_iota(jnp.int32, (HEAD, width), 1), HEAD)
            free = count - HEAD
            parts = ([(0, s[:free])] if free else []) + [(free, jnp.where(key <= query, s[free:], -jnp.inf))]
        tall = []
        for row, part in parts:
            score_v[pl.ds(room(h, count) + row, part.shape[0]), lanes] = part
            tall.append(jnp.max(part.reshape(part.shape[0] // 8, 8, width), axis=0))
        top = jnp.max(functools.reduce(jnp.maximum, tall), axis=0, keepdims=True) * EXP2_SCALE
        tops[h, first] = jnp.maximum(top, max_v[h, :, lanes]) if merge else top

    def weight_phase(unit):
        h, start, count, first, width, causal = unit
        lanes = pl.ds(first, width)
        total = None
        for c in range(count // KEY_ROWS):
            rows = pl.ds(room(h, count) + c * KEY_ROWS, KEY_ROWS)
            w = jnp.exp2(score_v[rows, lanes] * EXP2_SCALE - tops[h, first])
            part = jnp.sum(w.reshape(KEY_ROWS // 8, 8, width), axis=0)
            total = part if total is None else total + part
            weight_v[rows, lanes] = w.astype(BF16)
        sums[h, first] = total

    def value_phase(unit):
        h, start, count, first, width, causal = unit
        lanes = pl.ds(first, width)
        acc = lax.dot_general(kv_v[h, pl.ds(start, count), pl.ds(HEAD, HEAD)], weight_v[pl.ds(room(h, count), count), lanes], (((0,), (0,)), ((), ())), preferred_element_type=F32)
        total = jnp.sum(sums[h, first], axis=0, keepdims=True)
        if merge:
            scale = jnp.exp2(max_v[h, :, lanes] - tops[h, first])
            total, acc = sum_v[h, :, lanes] * scale + total, acc_v[h, :, lanes] * scale + acc
        if not (merge and last):
            max_v[h, :, lanes], sum_v[h, :, lanes], acc_v[h, :, lanes] = tops[h, first], total, acc
        if last:
            vals = (acc / total).astype(BF16)
            for i in range(width // HEAD):
                half, g = divmod(first // HEAD + i, GROUP)
                o_v[h, pl.ds(half * HEAD, HEAD), pl.ds(g * HEAD, HEAD)] = vals[:, i * HEAD:(i + 1) * HEAD].T

    for i in range(len(units) + 2):
        if i < len(units):
            score_phase(units[i])
        if 0 <= i - 1 < len(units):
            weight_phase(units[i - 1])
        if 0 <= i - 2 < len(units):
            value_phase(units[i - 2])


def own_units(start):
    return [(h, start, (half + 1) * HEAD, half * QCOLS, QCOLS, True) for h in range(KV) for half in range(2)]


def block_units(heads, first, end):
    return [(h, first * ROWS, (end - first) * ROWS, 0, GROUP * ROWS, False) for h in heads]


def kernel(x_hbm, pos_hbm, g_hbm, wq_hbm, wk_hbm, wv_hbm, wo_hbm,
           out_v, k_out, v_out,
           pos_v, g_v, wkv_v, wq_v, h_v, gain_v, inv_v, cos_v, sin_v, kv_v, q_v, o_v, max_v, sum_v, acc_v, score_v, weight_v, precv, relay_v, cache_v,
           x_sem, small_sem, first_sem, wkv_sem, wq_sem, kv_send, kv_recv, p_send, p_recv, relay_send, relay_recv):
    tp, cp = lax.axis_index("tp"), lax.axis_index("cp")
    other = 1 - tp
    x_part, wkv_slice, wkv_rest, wq_part, wo_part, pos_copy, g_copy = copies(
        (x_hbm, pos_hbm, g_hbm, wq_hbm, wk_hbm, wv_hbm, wo_hbm, out_v, pos_v, g_v, wkv_v, wq_v, x_sem, small_sem, first_sem, wkv_sem, wq_sem))

    g_copy.start()
    for i in range(X_PARTS):
        x_part(i).start()
    pos_copy.start()
    for t in range(1):
        for copy in wkv_slice(t):
            copy.start()
    barrier = pltpu.get_barrier_semaphore()
    for t in range(2):
        for c in range(4):
            @pl.when((tp != t) | (cp != c))
            def _():
                pl.semaphore_signal(barrier, inc=1, device_id={"tp": t, "cp": c}, device_id_type=MESH)

    def normalise(i):
        rows = pl.ds(i * X_ROWS, X_ROWS)
        inv = inv_v[rows, :]
        for t in range(WIDTH // HEAD):
            lanes = pl.ds(t * HEAD, HEAD)
            h_v[rows, lanes] = (out_v[rows, lanes].astype(F32) * inv * gain_v[pl.ds(t, 1), :]).astype(BF16)

    g_copy.wait()
    gain_v[...] = g_v[...].astype(F32)
    for i in range(X_PARTS):
        x_part(i).wait()
        if i == 0:
            for t in range(1, SLICES):
                for copy in wkv_slice(t):
                    copy.start()
        if i == 2:
            for copy in wkv_rest:
                copy.start()
        rows = pl.ds(i * X_ROWS, X_ROWS)
        squares = None
        for t in range(WIDTH // HEAD):
            xf = out_v[rows, pl.ds(t * HEAD, HEAD)].astype(F32)
            squares = xf * xf if squares is None else squares + xf * xf
        mean = jnp.sum(squares, axis=-1, keepdims=True) * (1.0 / WIDTH)
        if i:
            normalise(i - 1)
        inv_v[rows, :] = jnp.broadcast_to(lax.rsqrt(mean + EPS), (X_ROWS, HEAD))
    normalise(X_PARTS - 1)

    def piece(block, h):
        return kv_v.at[h, pl.ds(pl.multiple_of(block * ROWS, ROWS), ROWS), :]

    def kv_copy(src_block, h, target):
        return pltpu.make_async_remote_copy(
            src_ref=piece(src_block, h), dst_ref=piece(src_block, h), send_sem=kv_send,
            recv_sem=kv_recv.at[src_block, h], device_id={"cp": target}, device_id_type=MESH)

    def heads_of(acc, pair):
        for a in range(2):
            h = 2 * pair + a
            k = rope(acc[:, a * HEAD:(a + 1) * HEAD], cos_v[...], sin_v[...]).astype(BF16)
            piece(cp, h)[:, pl.ds(0, HEAD)] = k
            piece(cp, h)[:, pl.ds(HEAD, HEAD)] = acc[:, PAIR + a * HEAD:PAIR + (a + 1) * HEAD].astype(BF16)

    def send_heads(pair):
        for h in (2 * pair, 2 * pair + 1):
            @pl.when(cp == 0)
            def _():
                kv_copy(0, h, 2).start()
                kv_copy(0, h, 1).start()

            @pl.when(cp == 1)
            def _():
                kv_copy(1, h, 3).start()

            @pl.when(cp == 2)
            def _():
                kv_copy(2, h, 3).start()

    def query_heads(acc, j):
        for g in range(GROUP):
            q = rope(acc[:, g * HEAD:(g + 1) * HEAD], cos_v[...], sin_v[...]).astype(BF16)
            for half in range(2):
                q_v[j, pl.ds(half * QCOLS + g * HEAD, HEAD), :] = q[half * HEAD:(half + 1) * HEAD]

    pos_copy.wait()
    acc = None
    for part in range(4):
        for t in range(part * SLICES // 4, (part + 1) * SLICES // 4):
            wait_bytes(wkv_v.at[0, pl.ds(t * SLICE_ROWS, SLICE_ROWS), :], first_sem.at[t])
        if part == 0:
            wq_part(0).start()
        deep = pl.ds(part * WIDTH // 4, WIDTH // 4)
        d = jnp.dot(h_v[:, deep], wkv_v[0, deep, :], preferred_element_type=F32)
        acc = d if acc is None else acc + d
        if part == 0:
            rope_tables(pos_v, cos_v, sin_v)
    wq_part(1).start()
    heads_of(acc, 0)
    pl.semaphore_wait(barrier, 7)
    send_heads(0)

    wait_bytes(wkv_v.at[1], wkv_sem)
    wq_part(2).start()
    pending = jnp.dot(h_v[...], wkv_v[1], preferred_element_type=F32)

    def forward_to(block, h, target):
        kv_copy(block, h, target).wait_recv()
        kv_copy(block, h, target).start()

    def forward(h):
        @pl.when(cp == 2)
        def _():
            forward_to(0, h, 3)

        @pl.when(cp == 3)
        def _():
            forward_to(1, h, 2)

    stats = (q_v, kv_v, o_v, max_v, sum_v, acc_v, score_v, weight_v)
    for j in range(KV):
        wq_part(j).wait()
        if j == 0:
            wq_part(3).start()
        acc = jnp.dot(h_v[...], wq_v[j], preferred_element_type=F32)
        if j == 0:
            heads_of(pending, 1)
            send_heads(1)
        else:
            query_heads(pending, j - 1)
        pending = acc
        for copy in wo_part(j):
            copy.start()
        if j == KV - 1:
            forward(0)
    query_heads(pending, KV - 1)
    attend(own_units(pl.multiple_of(cp * ROWS, ROWS)), False, True, *stats)
    forward(1)

    def arrive(src_block, h):
        kv_copy(src_block, h, 0).wait_recv()

    @pl.when(cp == 1)
    def _():
        for h in range(KV):
            arrive(0, h)
        attend(block_units(range(KV), 0, 1), True, True, *stats)

    @pl.when(cp == 2)
    def _():
        arrive(1, 0)
        arrive(1, 1)
        attend(block_units((0, 1), 0, 2), True, True, *stats)
        forward_to(0, 2, 3)
        arrive(1, 2)
        attend(block_units((2,), 0, 2), True, True, *stats)
        forward_to(0, 3, 3)
        arrive(1, 3)
        attend(block_units((3,), 0, 2), True, True, *stats)

    @pl.when(cp == 3)
    def _():
        for h in range(KV):
            arrive(2, h)
        attend(block_units((0, 1), 2, 3), True, False, *stats)
        forward_to(1, 2, 2)
        attend(block_units((2, 3), 2, 3), True, False, *stats)
        arrive(0, 0)
        attend(block_units((0,), 0, 2), True, True, *stats)
        forward_to(1, 3, 2)
        arrive(0, 1)
        arrive(0, 2)
        attend(block_units((1, 2), 0, 2), True, True, *stats)
        arrive(0, 3)
        attend(block_units((3,), 0, 2), True, True, *stats)

    def sent(n):
        return wkv_v.at[0, pl.ds(pl.multiple_of(n * ROWS, ROWS), ROWS), pl.ds(0, OCHUNK)]

    def group(n):
        early = (n + 1) // 4
        return jnp.where(n < 14, early, n - 10) if not isinstance(n, int) else (early if n < 14 else n - 10)

    def p_copy(n):
        return pltpu.make_async_remote_copy(
            src_ref=sent(n), dst_ref=precv.at[n], send_sem=p_send, recv_sem=p_recv.at[group(n)],
            device_id={"tp": other}, device_id_type=MESH)

    def held(me, i):
        return pl.ds(sum(DETOUR_ROWS[me][:i]), DETOUR_ROWS[me][i])

    def relay_in(me, i):
        return pltpu.make_async_remote_copy(
            src_ref=sent(i).at[pl.ds(0, DETOUR_ROWS[me][i])], dst_ref=relay_v.at[held(me, i)], send_sem=p_send, recv_sem=relay_recv,
            device_id={"tp": other, "cp": 4 - me}, device_id_type=MESH)

    def relay_out(me, i):
        return pltpu.make_async_remote_copy(
            src_ref=relay_v.at[held(me, i)], dst_ref=precv.at[i, pl.ds(0, DETOUR_ROWS[me][i])], send_sem=relay_send, recv_sem=p_recv.at[group(i)],
            device_id={"cp": me}, device_id_type=MESH)

    def rest(me, i):
        rows = pl.ds(DETOUR_ROWS[me][i], ROWS - DETOUR_ROWS[me][i])
        return pltpu.make_async_remote_copy(
            src_ref=sent(i).at[rows], dst_ref=precv.at[i, rows], send_sem=p_send, recv_sem=p_recv.at[group(i)],
            device_id={"tp": other}, device_id_type=MESH)

    def pass_on(me):
        wait_bytes(relay_v.at[pl.ds(0, sum(DETOUR_ROWS[me]))], relay_recv)
        for i in range(len(DETOUR_ROWS[me])):
            relay_out(me, i).start()

    def passed_on(me):
        wait_bytes(relay_v.at[pl.ds(0, sum(DETOUR_ROWS[me]))], relay_send)

    @pl.loop(0, NOUT)
    def _(n):
        @pl.when(lax.rem(n, 4) == 0)
        def _():
            wait_bytes(wq_v.at[n // 4], wq_sem.at[n // 4])

        room = wo_room(wq_v, n)
        part = None
        for h in range(KV):
            d = jnp.dot(o_v[h], room[pl.ds(h * QCOLS, QCOLS), :], preferred_element_type=F32)
            part = d if part is None else part + d
        sent(n)[...] = part.astype(BF16)
        for me, detours in DETOUR_ROWS.items():
            for i in range(len(detours)):
                @pl.when((cp == me) & (n == i))
                def _():
                    relay_in(me, i).start()
                    if detours[i] < ROWS:
                        rest(me, i).start()

        direct = lax.rem(cp, 2) == 0
        for me, detours in DETOUR_ROWS.items():
            direct = direct | ((cp == me) & (n >= len(detours)))

        @pl.when(direct)
        def _():
            p_copy(n).start()

    @pl.when(cp == 3)
    def _():
        pass_on(1)

    for cache, lanes in ((k_out, pl.ds(0, HEAD)), (v_out, pl.ds(HEAD, HEAD))):
        for h in range(KV):
            cache_v[pl.ds(h, ROWS, stride=KV), :] = piece(cp, h)[:, lanes].astype(F32)
        cache[...] = cache_v[...].astype(BF16)

    @pl.when(lax.rem(cp, 2) == 0)
    def _():
        wait_bytes(kv_v.at[:, pl.ds(0, 2 * ROWS), :], kv_send)

    @pl.when(lax.rem(cp, 2) == 1)
    def _():
        wait_bytes(kv_v.at[:, pl.ds(0, ROWS), :], kv_send)

    def add_chunks(first, count):
        wait_bytes(precv.at[pl.ds(first, count)], p_recv.at[group(first)])
        for n in range(first, first + count):
            cols = pl.ds(n * OCHUNK, OCHUNK)
            total = sent(n)[...].astype(F32) + precv[n].astype(F32)
            out_v[:, cols] = (out_v[:, cols].astype(F32) + total).astype(BF16)

    add_chunks(3, 4)
    add_chunks(7, 4)

    @pl.when(cp == 1)
    def _():
        pass_on(3)

    @pl.when(cp == 3)
    def _():
        passed_on(1)

    add_chunks(11, 3)

    @pl.when(cp == 1)
    def _():
        passed_on(3)

    add_chunks(0, 3)
    add_chunks(14, 1)
    add_chunks(15, 1)
    wait_bytes(precv, p_send)


def store_results(out_v, k_v, v_v, out_hbm, k_hbm, v_hbm, sem):
    stores = [pltpu.make_async_copy(src, dst, sem.at[i]) for i, (src, dst) in enumerate(((out_v, out_hbm), (k_v, k_hbm), (v_v, v_hbm)))]
    for store in stores:
        store.start()
    for store in stores:
        store.wait()


def solution(mesh):
    row_spec = P(('dp', 'cp'), None)
    cache_spec = P(('dp', 'cp'), 'tp', None)
    head_cols = P(None, 'tp')

    def local_block(hidden, positions, norm_gain, w_query, w_key, w_value, w_out):
        dma = pltpu.SemaphoreType.DMA
        out, k_rope, v_heads = pl.pallas_call(
            kernel,
            out_shape=[
                jax.ShapeDtypeStruct((ROWS, WIDTH), BF16),
                jax.ShapeDtypeStruct((ROWS * KV, HEAD), BF16),
                jax.ShapeDtypeStruct((ROWS * KV, HEAD), BF16),
            ],
            in_specs=[pl.BlockSpec(memory_space=pltpu.HBM)] * 7,
            out_specs=[pl.BlockSpec(memory_space=pltpu.VMEM)] * 3,
            scratch_shapes=[
                pltpu.VMEM((ROWS,), jnp.int32),
                pltpu.VMEM((WIDTH // HEAD, HEAD), BF16),
                pltpu.VMEM((2, WIDTH, 2 * PAIR), BF16),
                pltpu.VMEM((KV, WIDTH, QCOLS), BF16),
                pltpu.VMEM((ROWS, WIDTH), BF16),
                pltpu.VMEM((WIDTH // HEAD, HEAD), F32),
                pltpu.VMEM((ROWS, HEAD), F32),
                pltpu.VMEM((ROWS, HEAD), F32),
                pltpu.VMEM((ROWS, HEAD), F32),
                pltpu.VMEM((KV, 4 * ROWS, 2 * HEAD), BF16),
                pltpu.VMEM((KV, GROUP * ROWS, HEAD), BF16),
                pltpu.VMEM((KV, ROWS, QCOLS), BF16),
                pltpu.VMEM((KV, 1, GROUP * ROWS), F32),
                pltpu.VMEM((KV, 1, GROUP * ROWS), F32),
                pltpu.VMEM((KV, HEAD, GROUP * ROWS), F32),
                pltpu.VMEM((KV * ROWS, GROUP * ROWS), F32),
                pltpu.VMEM((KV * ROWS, GROUP * ROWS), BF16),
                pltpu.VMEM((NOUT, ROWS, OCHUNK), BF16),
                pltpu.VMEM((max(map(sum, DETOUR_ROWS.values())), OCHUNK), BF16),
                pltpu.VMEM((ROWS * KV, HEAD), F32),
                dma((X_PARTS,)), dma((2,)), dma((SLICES,)), dma, dma((KV,)),
                dma, dma((3, KV)), dma, dma((6,)), dma, dma,
            ],
            compiler_params=pltpu.CompilerParams(collective_id=0, has_side_effects=True, vmem_limit_bytes=49 << 20),
        )(*(pltpu.with_memory_space_constraint(a, pltpu.HBM) for a in (hidden, positions, norm_gain.reshape(WIDTH // HEAD, HEAD), w_query, w_key, w_value, w_out)))
        out, k_rope, v_heads = pl.pallas_call(
            store_results,
            out_shape=[jax.ShapeDtypeStruct(a.shape, BF16) for a in (out, k_rope, v_heads)],
            in_specs=[pl.BlockSpec(memory_space=pltpu.VMEM)] * 3,
            out_specs=[pl.BlockSpec(memory_space=pl.ANY)] * 3,
            scratch_shapes=[dma((3,))],
            compiler_params=pltpu.CompilerParams(vmem_limit_bytes=4 << 20),
        )(out, k_rope, v_heads)
        return out, k_rope.reshape(ROWS, KV, HEAD), v_heads.reshape(ROWS, KV, HEAD)

    return jax.shard_map(local_block, mesh=mesh, in_specs=(row_spec, P(('dp', 'cp')), P(None), head_cols, head_cols, head_cols, P('tp', None)), out_specs=(row_spec, cache_spec, cache_spec), check_vma=False)
```
